32 devices in a mesh: rows: 16 (over z, y, x), cols: 2 (over core).
Axes of the slice: x: 2, y: 2, z: 4, core: 2. Of those that a mesh axis runs over, the one named last changes fastest.
Arguments:
- eigvecs: float32 [4096, 2048], P('rows', 'cols'), may hold values from -6 to 6
- reflectors: float32 [32, 4096], P('cols', 'rows'), may hold values from -17 to 17
- starts: int32 [32], replicated, may hold values from 0 to 63
Outputs:
- rotated: float32 [4096, 2048], P('rows', 'cols')
The draws below stay inside these ranges and needn't reach their ends.
Inputs may be any that keep to these rules, and one draw needn't show every extreme that they name: Sweep j's windows begin at rows starts[j] + k * 64.
All inputs are finite; a program needn't handle non-finite values.
Results may differ from the reference program's by a relative error of at most 0.00011.
Values sent between devices are 32-bit elements; how exact they have to be, the bound alone decides.
A program may use at most 64 MiB of HBM per device.

```python
import math
import jax
import jax.numpy as jnp
from jax import lax

BAND = 64
COLS = 2048
SWEEPS = 32
ORDER = 4096


def draw_reflectors(key, part):
    scale_key = jax.random.fold_in(key, 11)
    value_key = jax.random.fold_in(key, 12)
    extent = (SWEEPS, ORDER)
    scales = jnp.exp(jax.random.uniform(scale_key, extent, jnp.float32, math.log(0.3), math.log(3.0)))
    random_part = jnp.clip(jax.random.normal(value_key, extent, jnp.float32), -4.0, 4.0)
    return (random_part * scales).astype(jnp.float32)


def place_ends(values, key, low, high):
    longest = values.shape.index(max(values.shape))
    spots = []
    for shift in (0, 1):
        where = [jax.random.randint(jax.random.fold_in(key, axis), (), 0, length) for axis, length in enumerate(values.shape)]
        where[longest] = (where[longest] + shift) % values.shape[longest]
        spots.append(tuple(where))
    return values.at[spots[0]].set(low).at[spots[1]].set(high)


def levels(key, shape, cuts, smallest, high):
    loudness, own = 1.0, jax.random.fold_in(key, 6)
    for dim, parts in cuts:
        draws = jnp.exp(jax.random.uniform(jax.random.fold_in(own, dim), (parts,), jnp.float32, smallest / len(cuts), high / len(cuts)))
        loudness = loudness * jnp.repeat(draws, shape[dim] // parts).reshape([-1 if axis == dim else 1 for axis in range(len(shape))])
    return loudness


def centred(stream_key, dims, scale, limit, pieces=(), kind=jnp.bfloat16):
    result = scale * jax.random.normal(stream_key, dims, jnp.float32)
    if pieces:
        result = result * levels(stream_key, dims, pieces, -0.22, 0.18)
    return jnp.clip(result, -limit, limit).astype(kind)


def setup_inputs(seed: int = 0) -> dict:
    keys = jax.random.split(jax.random.key(seed), 4)
    eigvecs = centred(keys[0], (ORDER, COLS), 1.0, 6.0, ((0, 16), (1, 2)), jnp.float32)
    reflectors = draw_reflectors(jax.random.fold_in(keys[3], 71), 0)
    starts = place_ends(jax.random.randint(keys[2], (SWEEPS,), 0, BAND), jax.random.fold_in(keys[2], 1), 0, BAND - 1).astype(jnp.int32)
    return {"eigvecs": eigvecs, "reflectors": reflectors, "starts": starts}


def one_sweep(vectors, reflector, offset):
    total_rows = vectors.shape[0]
    blocks = total_rows // BAND
    rolled = jnp.roll(vectors, -offset, axis=0).reshape(blocks, BAND, vectors.shape[1])
    rolled_v = jnp.roll(reflector, -offset).reshape(blocks, BAND)
    squares = jnp.sum(rolled_v * rolled_v, axis=1)
    window = jnp.arange(blocks, dtype=jnp.int32)
    usable = (window + 1) * BAND + offset <= total_rows
    scaled = jnp.where(usable, 2.0 / jnp.where(usable, squares, 1.0), 0.0)
    products = jnp.einsum("kb,kbm->km", rolled_v, rolled, precision=lax.Precision.HIGHEST)
    rolled = rolled - rolled_v[:, :, None] * (scaled[:, None] * products)[:, None, :]
    return jnp.roll(rolled.reshape(total_rows, vectors.shape[1]), offset, axis=0)


def reference(eigvecs, reflectors, starts):
    def advance(sweep_idx, vectors):
        return one_sweep(vectors, reflectors[sweep_idx], starts[sweep_idx])
    return lax.fori_loop(0, SWEEPS, advance, eigvecs)
```

```python
import functools
import jax
import jax.numpy as jnp
from jax import lax
from jax.experimental import pallas as pl
from jax.experimental.pallas import tpu as pltpu
from jax.sharding import PartitionSpec as P

BAND = 64
LANES = 128
MESH = pl.DeviceIdType.MESH


def halves(a):
    high = a.astype(jnp.bfloat16)
    return high, (a - high.astype(jnp.float32)).astype(jnp.bfloat16)


def product(a, b, ca=1, cb=0):
    def one(left, right):
        return lax.dot_general(
            left, right, (((ca,), (cb,)), ((), ())), preferred_element_type=jnp.float32)
    return one(a[0], b[0]) + (one(a[0], b[1]) + one(a[1], b[0]))


def dot(a, b, ca=1, cb=0):
    return product(halves(a), halves(b), ca, cb)


def gram(a, b):
    return product(a, b, 1, 1) + lax.dot_general(
        a[1], b[1], (((1,), (1,)), ((), ())), preferred_element_type=jnp.float32)


def lanes_of(a):
    return lax.broadcasted_iota(jnp.int32, a.shape, 1)


def sweep_pair(shape, sweeps):
    rows = lax.broadcasted_iota(jnp.int32, shape, 0) % sweeps
    cols = lax.broadcasted_iota(jnp.int32, shape, 1) % sweeps
    return rows, cols


def lower(full, sweeps):
    rows, cols = sweep_pair(full.shape, sweeps)
    return jnp.where(rows > cols, full, 0.0)


def on_diagonal(shape):
    return lax.broadcasted_iota(jnp.int32, shape, 0) == lax.broadcasted_iota(jnp.int32, shape, 1)


def inverse(full, sweeps):
    eye = on_diagonal(full.shape)
    diag = jnp.where(eye, full, 0.0)
    down = jnp.sum(diag, axis=1, keepdims=True)
    across = jnp.sum(diag, axis=0, keepdims=True)
    down = 1.0 / jnp.where(down == 0.0, 1.0, down)
    across = 1.0 / jnp.where(across == 0.0, 1.0, across)
    rows, cols = sweep_pair(full.shape, sweeps)
    apart = rows ^ cols
    done = jnp.where(eye, down, 0.0)
    done = done - down * jnp.where((apart == 1) & (rows > cols), full, 0.0) * across
    size = 2
    while size < sweeps:
        reach = min(4 * size, sweeps)
        off = jnp.where((apart >= size) & (apart < reach) & (rows > cols), full, 0.0)
        inner = halves(done)
        step = halves(product(inner, halves(off)))
        first = done - product(step, inner)
        if reach > 2 * size:
            twice = product(step, step)
            first = first + dot(twice, first)
        done = first
        size = reach
    return done


def kernel(nrows, ncols, x_hbm, v_hbm, starts_hbm, out_ref, x_ref, v_all, starts_ref, lt_in, p_out,
           p_in, ltp_ref, ltp_in, q_ref, near_in, far_in, y_all, y_in, ax_ref, x_sem, s_sem, v_local,
           v_send, v_recv, l_send, l_recv, p_send, p_recv, b_send, b_recv, q_send, q_recv, y_send, y_recv):
    d, c = lax.axis_index("rows"), lax.axis_index("cols")
    own = v_hbm.shape[0]
    sweeps = v_all.shape[0]
    height, width = x_ref.shape
    depth = height // BAND
    team = p_in.shape[0]
    part = width // team
    half = sweeps // 2
    group, member = d // team, d % team
    groups = nrows // team
    place = v_all.at[pl.ds(pl.multiple_of(c * own, own), own)]
    mine = pltpu.make_async_copy(v_hbm, place, v_local)
    mine.start()
    begins = pltpu.make_async_copy(starts_hbm, starts_ref, s_sem)
    begins.start()
    load = pltpu.make_async_copy(x_hbm, x_ref, x_sem)
    load.start()

    offsets = (-2, -1, 1, 2)

    def there(offset):
        return group + offset >= 0 if offset < 0 else group + offset < groups

    def mate(step):
        return (member + step) % team

    barrier = pltpu.get_barrier_semaphore()
    for step in range(1, ncols):
        pl.semaphore_signal(barrier, inc=1, device_id=(d, (c + step) % ncols), device_id_type=MESH)
    for step in range(1, team):
        pl.semaphore_signal(
            barrier, inc=1, device_id=(group * team + mate(step), c), device_id_type=MESH)
    for offset in offsets:
        @pl.when(there(offset))
        def _():
            pl.semaphore_signal(barrier, inc=1, device_id=(d + offset * team, c), device_id_type=MESH)
    for i, offset in enumerate(offsets):
        @pl.when(jnp.logical_not(there(offset)))
        def _():
            ltp_in[i] = jnp.zeros_like(ltp_in[i])
            if abs(offset) == 1:
                near_in[i - 1] = jnp.zeros_like(near_in[0])
            else:
                far_in[i // 3] = jnp.zeros_like(far_in[0])
    peers = sum(there(offset).astype(jnp.int32) for offset in offsets)
    mine.wait()
    pl.semaphore_wait(barrier, peers + (ncols - 1) + (team - 1))

    copies = []
    for step in range(1, ncols):
        copy = pltpu.make_async_remote_copy(
            src_ref=place, dst_ref=place, send_sem=v_send.at[step - 1], recv_sem=v_recv.at[step - 1],
            device_id=(d, (c + step) % ncols), device_id_type=MESH)
        copy.start()
        copies.append(copy)
    begins.wait()
    across = jnp.broadcast_to(starts_ref[...], (sweeps, sweeps))
    begin = jnp.sum(jnp.where(on_diagonal(across.shape), across, 0), axis=1, keepdims=True)
    load.wait()
    x_halves = halves(x_ref[...])
    for copy in copies:
        copy.wait()

    v = v_all[...]
    row = lax.broadcasted_iota(jnp.int32, v.shape, 1)
    window = (row - begin + BAND) // BAND
    outside = ((window == 0) & (d == 0)) | ((window == depth) & (d == nrows - 1) & (begin > 0))
    v = jnp.where(outside, 0.0, v)
    parts = [jnp.where(window == k, v, 0.0) for k in range(depth + 1)]
    u_s = jnp.concatenate([parts[0], parts[depth]], axis=0)
    u_i = jnp.concatenate(parts[1:depth], axis=0)
    inside = u_i.shape[0]
    edge = 2 * sweeps
    half_s = 0.5 * jnp.sum(u_s * u_s, axis=1, keepdims=True)
    half_i = 0.5 * jnp.sum(u_i * u_i, axis=1, keepdims=True)
    pad = jnp.zeros((LANES - edge, height), jnp.float32)
    us_pad = halves(jnp.concatenate([u_s, pad], axis=0))
    us_h, ui_h = halves(u_s), halves(u_i)
    g_ii = gram(ui_h, ui_h)
    n_is = lower(gram(ui_h, us_pad), sweeps)
    n_si = lower(gram(us_h, ui_h), sweeps)
    g_ss = gram(us_h, us_pad)
    l_ii = jnp.where(on_diagonal(g_ii.shape), half_i, lower(g_ii, sweeps))
    n_ss = jnp.where(on_diagonal(g_ss.shape), half_s, lower(g_ss, sweeps))
    t = inverse(l_ii, sweeps)
    t_h, nis_h = halves(t), halves(n_is)
    k_h = halves(product(halves(n_si), t_h))
    lt_in[member] = n_ss - product(k_h, nis_h)

    def to_mate(step, src, dst, send, recv):
        return pltpu.make_async_remote_copy(
            src_ref=src, dst_ref=dst, send_sem=send.at[step - 1], recv_sem=recv.at[step - 1],
            device_id=(group * team + mate(step), c), device_id_type=MESH)

    def lt_copy(step):
        return to_mate(step, lt_in.at[member], lt_in.at[member], l_send, l_recv)

    def p_copy(step):
        return to_mate(step, p_out.at[mate(step)], p_in.at[member], p_send, p_recv)

    def y_copy(step):
        return to_mate(step, y_all.at[pl.ds(mate(step), 2)], y_in.at[member], y_send, y_recv)

    def to_group(i, src, dst, send, recv, slot):
        return pltpu.make_async_remote_copy(
            src_ref=src, dst_ref=dst, send_sem=send.at[i], recv_sem=recv.at[slot],
            device_id=(d + offsets[i] * team, c), device_id_type=MESH)

    def b_copy(i, slot):
        return to_group(i, ltp_ref, ltp_in.at[slot], b_send, b_recv, slot)

    def q_copy(i, slot):
        if offsets[i] == -2:
            src, dst = q_ref.at[0], far_in.at[1]
        elif offsets[i] == -1:
            src, dst = q_ref.at[pl.ds(0, 3)], near_in.at[1]
        elif offsets[i] == 1:
            src, dst = q_ref.at[pl.ds(2, 3)], near_in.at[0]
        else:
            src, dst = q_ref.at[2], far_in.at[0]
        return to_group(i, src, dst, q_send, q_recv, slot)

    for step in range(1, team):
        lt_copy(step).start()

    w_i = product(ui_h, x_halves)
    wi_h = halves(w_i)
    p = product(us_h, x_halves) - product(k_h, wi_h)
    for j in range(team):
        p_out[j] = p[:, j * part:(j + 1) * part]
    for step in range(1, team):
        p_copy(step).start()
    p_in[member] = p_out[member]

    u_t = u_i.T
    ut_h = halves(u_t)
    inner = product(t_h, wi_h)
    ax_ref[...] = x_ref[...] - product(ut_h, halves(inner))
    f = product(t_h, nis_h)[:, :edge]
    cm_h = halves(u_s.T - product(ut_h, halves(f)))
    cm3 = jnp.concatenate([cm_h[0], cm_h[1], cm_h[0]], axis=1)

    for step in range(1, team):
        lt_copy(step).wait_recv()
    turned = [lt_in[j] if j == 0 else pltpu.roll(lt_in[j], j * sweeps, 1) for j in range(team)]
    blocks = [turned[0][:sweeps]]
    for j in range(1, team):
        blocks.append(turned[j - 1][sweeps:] + turned[j][:sweeps])
    blocks.append(turned[team - 1][sweeps:])
    first = lanes_of(blocks[0]) < sweeps
    keep = [jnp.where(first, 0.0, block) for block in blocks]
    ends = [jnp.where(first, block, 0.0) for block in blocks]
    zero = jnp.zeros((sweeps, LANES), jnp.float32)
    m_ii = jnp.concatenate([zero] + keep[1:team], axis=0)
    m_si = jnp.concatenate([keep[0], keep[team]], axis=0)
    left = [zero] * team
    left[1] = left[1] + ends[1]
    left[team - 1] = left[team - 1] + pltpu.roll(ends[team - 1], sweeps, 1)
    m_is = jnp.concatenate(left, axis=0)
    m_ss = jnp.concatenate([ends[0], pltpu.roll(ends[team], sweeps, 1)], axis=0)
    tt_h = halves(inverse(m_ii, sweeps))
    mis_h = halves(m_is)
    kk_h = halves(product(halves(m_si), tt_h))
    ltp = m_ss - product(kk_h, mis_h)
    ltp_ref[...] = ltp
    for i, offset in enumerate(offsets):
        @pl.when(there(offset))
        def _():
            b_copy(i, 3 - i).start()
    ff_h = halves(product(tt_h, mis_h))

    for step in range(1, team):
        p_copy(step).wait_recv()
    sums = [jnp.zeros((sweeps, part), jnp.float32)]
    for j in range(1, team):
        sums.append(p_in[j - 1, sweeps:] + p_in[j, :sweeps])
    q_i = halves(jnp.concatenate(sums, axis=0))
    q_s = jnp.concatenate([p_in[0, :sweeps], p_in[team - 1, sweeps:]], axis=0)
    q = q_s - product(kk_h, q_i)
    for j in range(4):
        q_ref[j] = q[j * half:(j + 1) * half]
    q_ref[4] = q[:half]
    for i, offset in enumerate(offsets):
        @pl.when(there(offset))
        def _():
            q_copy(i, 3 - i).start()
    z_i = product(tt_h, q_i)

    for i, offset in enumerate(offsets):
        @pl.when(there(offset))
        def _():
            b_copy(i, i).wait_recv()
    far_l = jnp.where((lanes_of(zero) >= sweeps) & (lanes_of(zero) < edge), ltp_in[0, sweeps:], 0.0)
    far_r = jnp.where(first, ltp_in[3, :sweeps], 0.0)
    here = pltpu.roll(ltp_ref[...], sweeps, 1)
    near_l = ltp_in[1]
    near_r = pltpu.roll(ltp_in[2], 2 * sweeps, 1)
    big = jnp.concatenate([
        near_l[:sweeps] + pltpu.roll(far_l, LANES - sweeps, 1),
        near_l[sweeps:] + here[:sweeps],
        here[sweeps:] + near_r[:sweeps],
        near_r[sweeps:] + pltpu.roll(far_r, LANES - sweeps, 1),
    ], axis=0)
    s_h = halves(inverse(big, sweeps)[sweeps:3 * sweeps])

    for i, offset in enumerate(offsets):
        @pl.when(there(offset))
        def _():
            q_copy(i, i).wait_recv()
    none = jnp.zeros((half, part), jnp.float32)
    rhs = jnp.concatenate([
        far_in[0] + near_in[0, 2],
        none,
        near_in[0, 0] + q_ref[0],
        near_in[0, 1] + q_ref[1],
        q_ref[2] + near_in[1, 0],
        q_ref[3] + near_in[1, 1],
        near_in[1, 2] + far_in[1],
        none,
    ], axis=0)
    y_s = product(s_h, halves(rhs))
    y_pad = jnp.concatenate([y_s, jnp.zeros((LANES - edge, part), jnp.float32)], axis=0)
    y_i = z_i - product(ff_h, halves(y_pad))
    y_all[0] = y_s[:sweeps]
    for j in range(1, team):
        y_all[j] = y_i[j * sweeps:(j + 1) * sweeps]
    y_all[team] = y_s[sweeps:]
    for step in range(1, team):
        y_copy(step).start()

    def apply(j, y):
        y_h = halves(y)
        y3 = jnp.concatenate([y_h[0], y_h[0], y_h[1]], axis=0)
        cols = pl.ds(pl.multiple_of(j * part, part), part)
        out_ref[:, cols] = ax_ref[:, cols] - lax.dot_general(
            cm3, y3, (((1,), (0,)), ((), ())), preferred_element_type=jnp.float32)

    apply(member, y_all[pl.ds(member, 2)].reshape(edge, part))
    for step in range(1, team):
        y_copy(step).wait_recv()
        source = mate(team - step)
        apply(source, y_in[source].reshape(edge, part))

    for step in range(1, team):
        lt_copy(step).wait_send()
        p_copy(step).wait_send()
        y_copy(step).wait_send()
    for i, offset in enumerate(offsets):
        @pl.when(there(offset))
        def _():
            b_copy(i, 3 - i).wait_send()
            q_copy(i, 3 - i).wait_send()


def per_device(nrows, ncols, eigvecs, reflectors, starts):
    height, width = eigvecs.shape
    sweeps = starts.shape[0]
    team = sweeps // (2 * (height // BAND))
    part = width // team
    assert team * sweeps == LANES and nrows % team == 0
    f32 = jnp.float32
    hbm = pl.BlockSpec(memory_space=pltpu.HBM)
    dma = pltpu.SemaphoreType.DMA
    return pl.pallas_call(
        functools.partial(kernel, nrows, ncols),
        out_shape=jax.ShapeDtypeStruct((height, width), f32),
        in_specs=[hbm, hbm, hbm],
        out_specs=pl.BlockSpec(memory_space=pltpu.VMEM),
        scratch_shapes=[
            pltpu.VMEM((height, width), f32),
            pltpu.VMEM((sweeps, height), f32),
            pltpu.VMEM((1, sweeps), jnp.int32),
            pltpu.VMEM((team, 2 * sweeps, LANES), f32),
            pltpu.VMEM((team, 2 * sweeps, part), f32),
            pltpu.VMEM((team, 2 * sweeps, part), f32),
            pltpu.VMEM((2 * sweeps, LANES), f32),
            pltpu.VMEM((4, 2 * sweeps, LANES), f32),
            pltpu.VMEM((5, sweeps // 2, part), f32),
            pltpu.VMEM((2, 3, sweeps // 2, part), f32),
            pltpu.VMEM((2, sweeps // 2, part), f32),
            pltpu.VMEM((team + 1, sweeps, part), f32),
            pltpu.VMEM((team, 2, sweeps, part), f32),
            pltpu.VMEM((height, width), f32),
            dma, dma, dma,
            dma((ncols - 1,)), dma((ncols - 1,)),
            dma((team - 1,)), dma((team - 1,)),
            dma((team - 1,)), dma((team - 1,)),
            dma((4,)), dma((4,)),
            dma((4,)), dma((4,)),
            dma((team - 1,)), dma((team - 1,)),
        ],
        compiler_params=pltpu.CompilerParams(
            collective_id=0, has_side_effects=True, vmem_limit_bytes=32 * 1024 * 1024),
    )(*(pltpu.with_memory_space_constraint(a, pltpu.HBM)
        for a in (eigvecs, reflectors, starts.reshape(1, sweeps))))


def solution(mesh):
    in_specs = (P("rows", "cols"), P("cols", "rows"), P())
    out_specs = P("rows", "cols")
    body = functools.partial(per_device, mesh.shape["rows"], mesh.shape["cols"])
    return jax.shard_map(
        body, mesh=mesh, in_specs=in_specs, out_specs=out_specs, check_vma=False
    )
```

```python
import functools
import jax
import jax.numpy as jnp
from jax import lax
from jax.experimental import pallas as pl
from jax.experimental.pallas import tpu as pltpu
from jax.sharding import PartitionSpec as P

BAND = 64
LANES = 128
MESH = pl.DeviceIdType.MESH


def halves(a):
    high = a.astype(jnp.bfloat16)
    return high, (a - high.astype(jnp.float32)).astype(jnp.bfloat16)


def product(a, b, ca=1, cb=0):
    def one(left, right):
        return lax.dot_general(
            left, right, (((ca,), (cb,)), ((), ())), preferred_element_type=jnp.float32)
    return one(a[0], b[0]) + (one(a[0], b[1]) + one(a[1], b[0]))


def exact(a, b, ca=1, cb=0):
    return product(a, b, ca, cb) + lax.dot_general(
        a[1], b[1], (((ca,), (cb,)), ((), ())), preferred_element_type=jnp.float32)


def gram(a, b):
    return exact(a, b, 1, 1)


def packed(a, sweeps):
    return a[:sweeps] + pltpu.roll(a[sweeps:], 2 * sweeps, 1)


def unpacked(a, sweeps):
    first = lanes_of(a) < 2 * sweeps
    return jnp.where(first, a, 0.0), jnp.where(first, pltpu.roll(a, 2 * sweeps, 1), 0.0)


def turn(a, by):
    return pltpu.roll(a, by % LANES, 1) if by % LANES else a


def lanes_of(a):
    return lax.broadcasted_iota(jnp.int32, a.shape, 1)


def sweep_pair(shape, sweeps):
    rows = lax.broadcasted_iota(jnp.int32, shape, 0) % sweeps
    cols = lax.broadcasted_iota(jnp.int32, shape, 1) % sweeps
    return rows, cols


def lower(full, sweeps):
    rows, cols = sweep_pair(full.shape, sweeps)
    return jnp.where(rows > cols, full, 0.0)


def on_diagonal(shape):
    return lax.broadcasted_iota(jnp.int32, shape, 0) == lax.broadcasted_iota(jnp.int32, shape, 1)


def inverse(full, sweeps):
    eye = on_diagonal(full.shape)
    diag = jnp.where(eye, full, 0.0)
    down = jnp.sum(diag, axis=1, keepdims=True)
    across = jnp.sum(diag, axis=0, keepdims=True)
    down = 1.0 / jnp.where(down == 0.0, 1.0, down)
    across = 1.0 / jnp.where(across == 0.0, 1.0, across)
    rows, cols = sweep_pair(full.shape, sweeps)
    apart = rows ^ cols
    done = jnp.where(eye, down, 0.0)
    done = done - down * jnp.where((apart == 1) & (rows > cols), full, 0.0) * across
    size = 2
    while size < sweeps:
        reach = min(4 * size, sweeps)
        off = jnp.where((apart >= size) & (apart < reach) & (rows > cols), full, 0.0)
        inner = halves(done)
        step = halves(exact(inner, halves(off)))
        first = done - exact(step, inner)
        if reach > 2 * size:
            twice = exact(step, step)
            first = first + exact(halves(twice), halves(first))
        done = first
        size = reach
    return done


def kernel(nrows, ncols, x_hbm, v_hbm, starts_hbm, out_ref, x_ref, v_all, starts_ref, lt_in, p_out,
           p_in, ltp_ref, ltp_in, follow, q_ref, near_in, far_in, z_all, z_in, y_in, ax_ref, x_sem, s_sem, v_local,
           v_send, v_recv, l_send, l_recv, p_send, p_recv, b_send, b_recv, q_send, q_recv, z_send, z_recv,
           y_send, y_recv, entered, arrived):
    d, c = lax.axis_index("rows"), lax.axis_index("cols")
    own = v_hbm.shape[0]
    sweeps = v_all.shape[0]
    height, width = x_ref.shape
    depth = height // BAND
    team = p_in.shape[0]
    part = width // team
    half = sweeps // 2
    group, member = d // team, d % team
    groups = nrows // team
    place = v_all.at[pl.ds(pl.multiple_of(c * own, own), own)]
    mine = pltpu.make_async_copy(v_hbm, place, v_local)
    mine.start()
    begins = pltpu.make_async_copy(starts_hbm, starts_ref, s_sem)
    begins.start()
    load = pltpu.make_async_copy(x_hbm, x_ref, x_sem)
    load.start()

    offsets = (-2, -1, 1, 2)

    def there(offset):
        return group + offset >= 0 if offset < 0 else group + offset < groups

    def mate(step):
        return (member + step) % team

    last = ncols - 1
    barrier = pltpu.get_barrier_semaphore()
    for step in range(team):
        @pl.when((c != last) | (step > 0))
        def _():
            pl.semaphore_signal(
                barrier, inc=1, device_id=(group * team + mate(step), last), device_id_type=MESH)
    for offset in offsets:
        @pl.when(there(offset))
        def _():
            pl.semaphore_signal(barrier, inc=1, device_id=(d + offset * team, 0), device_id_type=MESH)
    z_all[0] = jnp.zeros_like(z_all[0])
    z_all[team] = jnp.zeros_like(z_all[0])
    for i, offset in enumerate(offsets):
        @pl.when(jnp.logical_not(there(offset)))
        def _():
            ltp_in[i] = jnp.zeros_like(ltp_in[i])
            if abs(offset) == 1:
                near_in[i - 1] = jnp.zeros_like(near_in[0])
            else:
                far_in[i // 3] = jnp.zeros_like(far_in[0])
    mine.wait()

    @pl.when(c == last)
    def _():
        pl.semaphore_wait(barrier, ncols * team - 1)
        for step in range(1, ncols):
            pl.semaphore_signal(entered, inc=1, device_id=(d, (c + step) % ncols), device_id_type=MESH)

    @pl.when(c != last)
    def _():
        pl.semaphore_wait(entered, 1)

    copies = []
    for step in range(1, ncols):
        copy = pltpu.make_async_remote_copy(
            src_ref=place, dst_ref=place, send_sem=v_send.at[step - 1], recv_sem=v_recv.at[step - 1],
            device_id=(d, (c + step) % ncols), device_id_type=MESH)
        copy.start()
        copies.append(copy)
    begins.wait()
    across = jnp.broadcast_to(starts_ref[...], (sweeps, sweeps))
    begin = jnp.sum(jnp.where(on_diagonal(across.shape), across, 0), axis=1, keepdims=True)
    load.wait()
    x_halves = halves(x_ref[...])
    for copy in copies:
        copy.wait_recv()

    v = v_all[...]
    row = lax.broadcasted_iota(jnp.int32, v.shape, 1)
    window = (row - begin + BAND) // BAND
    outside = ((window == 0) & (d == 0)) | ((window == depth) & (d == nrows - 1) & (begin > 0))
    v = jnp.where(outside, 0.0, v)
    parts = [jnp.where(window == k, v, 0.0) for k in range(depth + 1)]
    u_s = jnp.concatenate([parts[0], parts[depth]], axis=0)
    u_i = jnp.concatenate(parts[1:depth], axis=0)
    inside = u_i.shape[0]
    edge = 2 * sweeps
    half_s = 0.5 * jnp.sum(u_s * u_s, axis=1, keepdims=True)
    half_i = 0.5 * jnp.sum(u_i * u_i, axis=1, keepdims=True)
    pad = jnp.zeros((LANES - edge, height), jnp.float32)
    us_pad = halves(jnp.concatenate([u_s, pad], axis=0))
    us_h, ui_h = halves(u_s), halves(u_i)
    g_ii = gram(ui_h, ui_h)
    n_is = lower(gram(ui_h, us_pad), sweeps)
    n_si = lower(gram(us_h, ui_h), sweeps)
    g_ss = gram(us_h, us_pad)
    l_ii = jnp.where(on_diagonal(g_ii.shape), half_i, lower(g_ii, sweeps))
    n_ss = jnp.where(on_diagonal(g_ss.shape), half_s, lower(g_ss, sweeps))
    wi_h = halves(product(ui_h, x_halves))
    w_s = product(us_h, x_halves)
    t = inverse(l_ii, sweeps)
    t_h, nis_h = halves(t), halves(n_is)
    k_h = halves(exact(halves(n_si), t_h))
    lt_in[member] = packed(n_ss - exact(k_h, nis_h), sweeps)

    def to_mate(step, src, dst, send, recv):
        return pltpu.make_async_remote_copy(
            src_ref=src, dst_ref=dst, send_sem=send.at[step - 1], recv_sem=recv.at[step - 1],
            device_id=(group * team + mate(step), c), device_id_type=MESH)

    def lt_copy(step):
        return to_mate(step, lt_in.at[member], lt_in.at[member], l_send, l_recv)

    def p_copy(step):
        return to_mate(step, p_out.at[mate(step)], p_in.at[member], p_send, p_recv)

    def z_copy(step):
        return to_mate(step, z_all.at[pl.ds(mate(step), 2)], z_in.at[member], z_send, z_recv)

    def y_copy(step):
        return to_mate(step, y_in.at[member], y_in.at[member], y_send, y_recv)

    def to_group(i, src, dst, send, recv, slot):
        return pltpu.make_async_remote_copy(
            src_ref=src, dst_ref=dst, send_sem=send.at[i], recv_sem=recv.at[slot],
            device_id=(d + offsets[i] * team, c), device_id_type=MESH)

    def b_copy(i, slot):
        return to_group(i, ltp_ref, ltp_in.at[slot], b_send, b_recv, slot)

    def q_copy(i, slot):
        if offsets[i] == -2:
            src, dst = q_ref.at[0], far_in.at[1]
        elif offsets[i] == -1:
            src, dst = q_ref.at[pl.ds(0, 3)], near_in.at[1]
        elif offsets[i] == 1:
            src, dst = q_ref.at[pl.ds(2, 3)], near_in.at[0]
        else:
            src, dst = q_ref.at[2], far_in.at[0]
        return to_group(i, src, dst, q_send, q_recv, slot)

    for step in range(1, team):
        lt_copy(step).start()

    p = w_s - product(k_h, wi_h)
    for j in range(team):
        p_out[j] = p[:, j * part:(j + 1) * part]
    for step in range(1, team):
        p_copy(step).start()
    p_in[member] = p_out[member]

    u_t = u_i.T
    ut_h = halves(u_t)
    inner = product(t_h, wi_h)
    ax_ref[...] = x_ref[...] - product(ut_h, halves(inner))
    f = exact(t_h, nis_h)[:, :edge]
    cm_h = halves(u_s.T - product(ut_h, halves(f)))

    for step in range(1, team):
        lt_copy(step).wait_recv()
    zero = jnp.zeros((sweeps, LANES), jnp.float32)
    blocks = [zero] * (team + 1)
    for j in range(team):
        for side, rows in enumerate(unpacked(lt_in[j], sweeps)):
            blocks[j + side] = blocks[j + side] + turn(rows, j * sweeps)
    first = lanes_of(blocks[0]) < sweeps
    keep = [jnp.where(first, 0.0, block) for block in blocks]
    ends = [jnp.where(first, block, 0.0) for block in blocks]
    m_ii = jnp.concatenate([zero] + keep[1:team], axis=0)
    m_si = jnp.concatenate([keep[0], keep[team]], axis=0)
    left = [zero] * team
    left[1] = left[1] + ends[1]
    left[team - 1] = left[team - 1] + pltpu.roll(ends[team - 1], sweeps, 1)
    m_is = jnp.concatenate(left, axis=0)
    m_ss = jnp.concatenate([ends[0], pltpu.roll(ends[team], sweeps, 1)], axis=0)
    tt_h = halves(inverse(m_ii, sweeps))
    mis_h = halves(m_is)
    kk_h = halves(exact(halves(m_si), tt_h))
    ltp_ref[...] = packed(m_ss - exact(kk_h, mis_h), sweeps)
    peers = sum(there(offset).astype(jnp.int32) for offset in offsets)

    @pl.when(c == 0)
    def _():
        pl.semaphore_wait(barrier, peers * ncols)
        for step in range(1, ncols):
            pl.semaphore_signal(arrived, inc=1, device_id=(d, step), device_id_type=MESH)

    @pl.when(c != 0)
    def _():
        pl.semaphore_wait(arrived, 1)

    for i, offset in enumerate(offsets):
        @pl.when(there(offset))
        def _():
            b_copy(i, 3 - i).start()
    ff = exact(tt_h, mis_h)
    at_left = jnp.where(on_diagonal(zero.shape), 1.0, 0.0)
    follow[0] = at_left
    for j in range(1, team):
        follow[j] = -ff[j * sweeps:(j + 1) * sweeps]
    follow[team] = turn(at_left, sweeps)
    mine_h = halves(follow[pl.ds(member, 2)].reshape(edge, LANES))
    cf_h = halves(product(cm_h, mine_h)[:, :edge])
    cf3 = jnp.concatenate([cf_h[0], cf_h[1], cf_h[0]], axis=1)

    for step in range(1, team):
        p_copy(step).wait_recv()
    sums = [jnp.zeros((sweeps, part), jnp.float32)]
    for j in range(1, team):
        sums.append(p_in[j - 1, sweeps:] + p_in[j, :sweeps])
    q_i = halves(jnp.concatenate(sums, axis=0))
    q_s = jnp.concatenate([p_in[0, :sweeps], p_in[team - 1, sweeps:]], axis=0)
    q = q_s - product(kk_h, q_i)
    for j in range(4):
        q_ref[j] = q[j * half:(j + 1) * half]
    q_ref[4] = q[:half]
    for i, offset in enumerate(offsets):
        @pl.when(there(offset))
        def _():
            q_copy(i, 3 - i).start()
    z_i = product(tt_h, q_i)
    for j in range(1, team):
        z_all[j] = z_i[j * sweeps:(j + 1) * sweeps]
    for step in range(1, team):
        z_copy(step).start()

    for i, offset in enumerate(offsets):
        @pl.when(there(offset))
        def _():
            b_copy(i, i).wait_recv()
    here = unpacked(ltp_ref[...], sweeps)
    near_l = unpacked(ltp_in[1], sweeps)
    near_r = unpacked(ltp_in[2], sweeps)
    far_l = unpacked(ltp_in[0], sweeps)[1]
    far_r = unpacked(ltp_in[3], sweeps)[0]
    big = jnp.concatenate([
        near_l[0] + turn(jnp.where(first, 0.0, far_l), -sweeps),
        near_l[1] + turn(here[0], sweeps),
        turn(here[1], sweeps) + turn(near_r[0], 2 * sweeps),
        turn(near_r[1], 2 * sweeps) + turn(jnp.where(first, far_r, 0.0), 3 * sweeps),
    ], axis=0)
    s_h = halves(inverse(big, sweeps)[sweeps:3 * sweeps])

    for i, offset in enumerate(offsets):
        @pl.when(there(offset))
        def _():
            q_copy(i, i).wait_recv()
    none = jnp.zeros((half, part), jnp.float32)
    rhs = jnp.concatenate([
        far_in[0] + near_in[0, 2],
        none,
        near_in[0, 0] + q_ref[0],
        near_in[0, 1] + q_ref[1],
        q_ref[2] + near_in[1, 0],
        q_ref[3] + near_in[1, 1],
        near_in[1, 2] + far_in[1],
        none,
    ], axis=0)
    y_s = product(s_h, halves(rhs))
    y_in[member] = y_s
    for step in range(1, team):
        y_copy(step).start()

    cm3 = jnp.concatenate([cm_h[0], cm_h[1], cm_h[0]], axis=1)

    def apply(left, y):
        y_h = halves(y)
        y3 = jnp.concatenate([y_h[0], y_h[0], y_h[1]], axis=0)
        return lax.dot_general(left, y3, (((1,), (0,)), ((), ())), preferred_element_type=jnp.float32)

    z_in[member] = z_all[pl.ds(member, 2)]
    for step in range(1, team):
        z_copy(step).wait_recv()
    for j in range(team):
        cols = slice(j * part, (j + 1) * part)
        ax_ref[:, cols] = ax_ref[:, cols] - apply(cm3, z_in[j].reshape(edge, part))

    def last_step(j):
        cols = pl.ds(pl.multiple_of(j * part, part), part)
        out_ref[:, cols] = ax_ref[:, cols] - apply(cf3, y_in[j])

    last_step(member)
    for step in range(1, team):
        y_copy(step).wait_recv()
        last_step(mate(team - step))

    for copy in copies:
        copy.wait_send()
    for step in range(1, team):
        lt_copy(step).wait_send()
        p_copy(step).wait_send()
        y_copy(step).wait_send()
        z_copy(step).wait_send()
    for i, offset in enumerate(offsets):
        @pl.when(there(offset))
        def _():
            b_copy(i, 3 - i).wait_send()
            q_copy(i, 3 - i).wait_send()


def per_device(nrows, ncols, eigvecs, reflectors, starts):
    height, width = eigvecs.shape
    sweeps = starts.shape[0]
    team = sweeps // (2 * (height // BAND))
    part = width // team
    assert team * sweeps == LANES and nrows % team == 0
    f32 = jnp.float32
    hbm = pl.BlockSpec(memory_space=pltpu.HBM)
    dma = pltpu.SemaphoreType.DMA
    return pl.pallas_call(
        functools.partial(kernel, nrows, ncols),
        out_shape=jax.ShapeDtypeStruct((height, width), f32),
        in_specs=[hbm, hbm, hbm],
        out_specs=pl.BlockSpec(memory_space=pltpu.VMEM),
        scratch_shapes=[
            pltpu.VMEM((height, width), f32),
            pltpu.VMEM((sweeps, height), f32),
            pltpu.VMEM((1, sweeps), jnp.int32),
            pltpu.VMEM((team, sweeps, LANES), f32),
            pltpu.VMEM((team, 2 * sweeps, part), f32),
            pltpu.VMEM((team, 2 * sweeps, part), f32),
            pltpu.VMEM((sweeps, LANES), f32),
            pltpu.VMEM((4, sweeps, LANES), f32),
            pltpu.VMEM((team + 1, sweeps, LANES), f32),
            pltpu.VMEM((5, sweeps // 2, part), f32),
            pltpu.VMEM((2, 3, sweeps // 2, part), f32),
            pltpu.VMEM((2, sweeps // 2, part), f32),
            pltpu.VMEM((team + 1, sweeps, part), f32),
            pltpu.VMEM((team, 2, sweeps, part), f32),
            pltpu.VMEM((team, 2 * sweeps, part), f32),
            pltpu.VMEM((height, width), f32),
            dma, dma, dma,
            dma((ncols - 1,)), dma((ncols - 1,)),
            dma((team - 1,)), dma((team - 1,)),
            dma((team - 1,)), dma((team - 1,)),
            dma((4,)), dma((4,)),
            dma((4,)), dma((4,)),
            dma((team - 1,)), dma((team - 1,)),
            dma((team - 1,)), dma((team - 1,)),
            pltpu.SemaphoreType.REGULAR, pltpu.SemaphoreType.REGULAR,
        ],
        compiler_params=pltpu.CompilerParams(
            collective_id=0, has_side_effects=True, vmem_limit_bytes=32 * 1024 * 1024),
    )(*(pltpu.with_memory_space_constraint(a, pltpu.HBM)
        for a in (eigvecs, reflectors, starts.reshape(1, sweeps))))


def solution(mesh):
    in_specs = (P("rows", "cols"), P("cols", "rows"), P())
    out_specs = P("rows", "cols")
    body = functools.partial(per_device, mesh.shape["rows"], mesh.shape["cols"])
    return jax.shard_map(
        body, mesh=mesh, in_specs=in_specs, out_specs=out_specs, check_vma=False
    )
```

```python
import functools
import jax
import jax.numpy as jnp
from jax import lax
from jax.experimental import pallas as pl
from jax.experimental.pallas import tpu as pltpu
from jax.sharding import PartitionSpec as P

BAND = 64
LANES = 128
MESH = pl.DeviceIdType.MESH


def halves(a):
    high = a.astype(jnp.bfloat16)
    return high, (a - high.astype(jnp.float32)).astype(jnp.bfloat16)


def product(a, b, ca=1, cb=0):
    def one(left, right):
        return lax.dot_general(
            left, right, (((ca,), (cb,)), ((), ())), preferred_element_type=jnp.float32)
    return one(a[0], b[0]) + (one(a[0], b[1]) + one(a[1], b[0]))


def exact(a, b, ca=1, cb=0):
    return product(a, b, ca, cb) + lax.dot_general(
        a[1], b[1], (((ca,), (cb,)), ((), ())), preferred_element_type=jnp.float32)


def gram(a, b):
    return exact(a, b, 1, 1)


def packed(a, sweeps):
    return a[:sweeps] + pltpu.roll(a[sweeps:], 2 * sweeps, 1)


def unpacked(a, sweeps):
    first = lanes_of(a) < 2 * sweeps
    return jnp.where(first, a, 0.0), jnp.where(first, pltpu.roll(a, 2 * sweeps, 1), 0.0)


def turn(a, by):
    return pltpu.roll(a, by % LANES, 1) if by % LANES else a


def lanes_of(a):
    return lax.broadcasted_iota(jnp.int32, a.shape, 1)


def sweep_pair(shape, sweeps):
    rows = lax.broadcasted_iota(jnp.int32, shape, 0) % sweeps
    cols = lax.broadcasted_iota(jnp.int32, shape, 1) % sweeps
    return rows, cols


def lower(full, sweeps):
    rows, cols = sweep_pair(full.shape, sweeps)
    return jnp.where(rows > cols, full, 0.0)


def on_diagonal(shape):
    return lax.broadcasted_iota(jnp.int32, shape, 0) == lax.broadcasted_iota(jnp.int32, shape, 1)


def seed(full, size):
    lanes = full.shape[1]
    eye = on_diagonal(full.shape)
    diag = jnp.where(eye, full, 0.0)
    down = jnp.sum(diag, axis=1, keepdims=True)
    across = jnp.sum(diag, axis=0, keepdims=True)
    down = 1.0 / jnp.where(down == 0.0, 1.0, down)
    across = 1.0 / jnp.where(across == 0.0, 1.0, across)
    rows = lax.broadcasted_iota(jnp.int32, full.shape, 0)
    cols = lax.broadcasted_iota(jnp.int32, full.shape, 1)
    scaled = jnp.where((rows ^ cols) < size, down * full, 0.0)
    below = [jnp.where(rows - cols == m, scaled, 0.0) for m in range(size)]
    below = [jnp.sum(entries, axis=0, keepdims=True) for entries in below]
    terms = [across]
    for k in range(1, size):
        total = below[k] * across
        for m in range(1, k):
            total = total + pltpu.roll(below[m], lanes - (k - m), 1) * terms[k - m]
        terms.append(-total)
    done = jnp.where(eye, across, 0.0)
    for k in range(1, size):
        done = jnp.where(rows - cols == k, terms[k], done)
    return done


def seed_pairs(full, sweeps):
    eye = on_diagonal(full.shape)
    diag = jnp.where(eye, full, 0.0)
    down = jnp.sum(diag, axis=1, keepdims=True)
    across = jnp.sum(diag, axis=0, keepdims=True)
    down = 1.0 / jnp.where(down == 0.0, 1.0, down)
    across = 1.0 / jnp.where(across == 0.0, 1.0, across)
    rows, cols = sweep_pair(full.shape, sweeps)
    pair = ((rows ^ cols) == 1) & (rows > cols)
    return jnp.where(eye, down, 0.0) - down * jnp.where(pair, full, 0.0) * across


def inverse(full, sweeps, size, done, right=None):
    rows, cols = sweep_pair(full.shape, sweeps)
    apart = rows ^ cols
    while size < sweeps:
        reach = min(4 * size, sweeps)
        off = jnp.where((apart >= size) & (apart < reach) & (rows > cols), full, 0.0)
        inner = halves(done)
        step = halves(exact(inner, halves(off)))
        if reach == sweeps and right is not None:
            done = jnp.concatenate([done, exact(inner, right)], axis=1)
            inner = halves(done)
        first = done - exact(step, inner)
        if reach > 2 * size:
            twice = exact(step, step)
            first = first + exact(halves(twice), halves(first))
        done = first
        size = reach
    if right is None:
        return done
    return done[:, :full.shape[1]], done[:, full.shape[1]:]


def kernel(nrows, ncols, x_hbm, v_hbm, starts_hbm, out_ref, x_ref, v_all, starts_ref, lt_in, p_out,
           p_in, ltp_ref, ltp_in, follow, q_ref, near_in, far_in, z_all, z_in, y_in, ax_ref, x_sem, s_sem, v_local,
           v_send, v_recv, l_send, l_recv, p_send, p_recv, b_send, b_recv, q_send, q_recv, z_send, z_recv,
           y_send, y_recv, paired, entered, arrived):
    d, c = lax.axis_index("rows"), lax.axis_index("cols")
    own = v_hbm.shape[0]
    sweeps = v_all.shape[0]
    height, width = x_ref.shape
    depth = height // BAND
    team = p_in.shape[0]
    part = width // team
    half = sweeps // 2
    group, member = d // team, d % team
    groups = nrows // team
    place = v_all.at[pl.ds(pl.multiple_of(c * own, own), own)]
    mine = pltpu.make_async_copy(v_hbm, place, v_local)
    mine.start()
    begins = pltpu.make_async_copy(starts_hbm, starts_ref, s_sem)
    begins.start()
    load = pltpu.make_async_copy(x_hbm, x_ref, x_sem)
    load.start()

    offsets = (-2, -1, 1, 2)

    def there(offset):
        return group + offset >= 0 if offset < 0 else group + offset < groups

    def mate(step):
        return (member + step) % team

    last = ncols - 1
    base = group * team
    barrier = pltpu.get_barrier_semaphore()

    def greet(sem, slab, core):
        pl.semaphore_signal(sem, inc=1, device_id=(slab, core), device_id_type=MESH)

    @pl.when(c > 0)
    def _():
        greet(barrier, d, 0)

    @pl.when((member > 0) | (c < last))
    def _():
        greet(barrier, base, last)
    for offset in offsets:
        @pl.when(there(offset))
        def _():
            greet(barrier, base + offset * team + team - 1, last)
    z_all[0] = jnp.zeros_like(z_all[0])
    z_all[team] = jnp.zeros_like(z_all[0])
    for i, offset in enumerate(offsets):
        @pl.when(jnp.logical_not(there(offset)))
        def _():
            ltp_in[i] = jnp.zeros_like(ltp_in[i])
            if abs(offset) == 1:
                near_in[i - 1] = jnp.zeros_like(near_in[0])
            else:
                far_in[i // 3] = jnp.zeros_like(far_in[0])
    mine.wait()

    @pl.when(c == 0)
    def _():
        pl.semaphore_wait(barrier, last)
        for core in range(1, ncols):
            greet(paired, d, core)

    @pl.when(c > 0)
    def _():
        pl.semaphore_wait(paired, 1)

    copies = []
    for step in range(1, ncols):
        copy = pltpu.make_async_remote_copy(
            src_ref=place, dst_ref=place, send_sem=v_send.at[step - 1], recv_sem=v_recv.at[step - 1],
            device_id=(d, (c + step) % ncols), device_id_type=MESH)
        copy.start()
        copies.append(copy)
    begins.wait()
    across = jnp.broadcast_to(starts_ref[...], (sweeps, sweeps))
    begin = jnp.sum(jnp.where(on_diagonal(across.shape), across, 0), axis=1, keepdims=True)
    load.wait()
    x_halves = halves(x_ref[...])
    for copy in copies:
        copy.wait_recv()

    v = v_all[...]
    row = lax.broadcasted_iota(jnp.int32, v.shape, 1)
    window = (row - begin + BAND) // BAND
    outside = ((window == 0) & (d == 0)) | ((window == depth) & (d == nrows - 1) & (begin > 0))
    v = jnp.where(outside, 0.0, v)
    parts = [jnp.where(window == k, v, 0.0) for k in range(depth + 1)]
    u_s = jnp.concatenate([parts[0], parts[depth]], axis=0)
    u_i = jnp.concatenate(parts[1:depth], axis=0)
    inside = u_i.shape[0]
    edge = 2 * sweeps
    half_s = 0.5 * jnp.sum(u_s * u_s, axis=1, keepdims=True)
    half_i = 0.5 * jnp.sum(u_i * u_i, axis=1, keepdims=True)
    half_i = jnp.concatenate([half_i, jnp.zeros((LANES - inside, 1), jnp.float32)], axis=0)
    pad = jnp.zeros((LANES - edge, height), jnp.float32)
    us_pad = halves(jnp.concatenate([u_s, pad], axis=0))
    ui_pad = halves(jnp.concatenate([u_i, jnp.zeros((LANES - inside, height), jnp.float32)], axis=0))
    us_h, ui_h = halves(u_s), halves(u_i)
    g_ii = gram(ui_pad, ui_pad)
    n_is = lower(gram(ui_pad, us_pad), sweeps)
    n_si = lower(gram(us_h, ui_pad), sweeps)
    g_ss = gram(us_h, us_pad)
    l_ii = jnp.where(on_diagonal(g_ii.shape), half_i, lower(g_ii, sweeps))
    n_ss = jnp.where(on_diagonal(g_ss.shape), half_s, lower(g_ss, sweeps))
    wi_h = halves(product(ui_h, x_halves))
    w_s = product(us_h, x_halves)
    t, f = inverse(l_ii, sweeps, 2, seed_pairs(l_ii, sweeps), halves(n_is))
    nsi_h = halves(n_si)
    lt_in[member] = packed(n_ss - exact(nsi_h, halves(f)), sweeps)
    t = t[:, :inside]
    k_h = halves(exact(nsi_h, halves(t)))
    t_h = halves(t[:inside])

    def to_mate(step, src, dst, send, recv):
        return pltpu.make_async_remote_copy(
            src_ref=src, dst_ref=dst, send_sem=send.at[step - 1], recv_sem=recv.at[step - 1],
            device_id=(group * team + mate(step), c), device_id_type=MESH)

    def lt_copy(step):
        return to_mate(step, lt_in.at[member], lt_in.at[member], l_send, l_recv)

    def p_copy(step):
        return to_mate(step, p_out.at[mate(step)], p_in.at[member], p_send, p_recv)

    def z_copy(step):
        return to_mate(step, z_all.at[pl.ds(mate(step), 2)], z_in.at[member], z_send, z_recv)

    def y_copy(step):
        return to_mate(step, y_in.at[member], y_in.at[member], y_send, y_recv)

    def to_group(i, src, dst, send, recv, slot):
        return pltpu.make_async_remote_copy(
            src_ref=src, dst_ref=dst, send_sem=send.at[i], recv_sem=recv.at[slot],
            device_id=(d + offsets[i] * team, c), device_id_type=MESH)

    def b_copy(i, slot):
        return to_group(i, ltp_ref, ltp_in.at[slot], b_send, b_recv, slot)

    def q_copy(i, slot):
        if offsets[i] == -2:
            src, dst = q_ref.at[0], far_in.at[1]
        elif offsets[i] == -1:
            src, dst = q_ref.at[pl.ds(0, 3)], near_in.at[1]
        elif offsets[i] == 1:
            src, dst = q_ref.at[pl.ds(2, 3)], near_in.at[0]
        else:
            src, dst = q_ref.at[2], far_in.at[0]
        return to_group(i, src, dst, q_send, q_recv, slot)

    @pl.when((member == 0) & (c == last))
    def _():
        pl.semaphore_wait(barrier, ncols * team - 1)
        for slab in range(team):
            for core in range(ncols):
                if slab > 0 or core < last:
                    greet(entered, base + slab, core)

    @pl.when((member > 0) | (c < last))
    def _():
        pl.semaphore_wait(entered, 1)

    for step in range(1, team):
        lt_copy(step).start()

    p = w_s - product(k_h, wi_h)
    for j in range(team):
        p_out[j] = p[:, j * part:(j + 1) * part]
    for step in range(1, team):
        p_copy(step).start()
    p_in[member] = p_out[member]

    peers = sum(there(offset).astype(jnp.int32) for offset in offsets)

    @pl.when((member == team - 1) & (c == last))
    def _():
        pl.semaphore_wait(barrier, peers * ncols * team)
        for slab in range(team):
            for core in range(ncols):
                if slab < team - 1 or core < last:
                    greet(arrived, base + slab, core)

    u_t = u_i.T
    ut_h = halves(u_t)
    inner = product(t_h, wi_h)
    ax_ref[...] = x_ref[...] - product(ut_h, halves(inner))
    cm_h = halves(u_s.T - product(ut_h, halves(f[:inside, :edge])))

    for step in range(1, team):
        lt_copy(step).wait_recv()
    zero = jnp.zeros((sweeps, LANES), jnp.float32)
    blocks = [zero] * (team + 1)
    for j in range(team):
        for side, rows in enumerate(unpacked(lt_in[j], sweeps)):
            blocks[j + side] = blocks[j + side] + turn(rows, j * sweeps)
    first = lanes_of(blocks[0]) < sweeps
    keep = [jnp.where(first, 0.0, block) for block in blocks]
    ends = [jnp.where(first, block, 0.0) for block in blocks]
    m_ii = jnp.concatenate([zero] + keep[1:team], axis=0)
    m_si = jnp.concatenate([keep[0], keep[team]], axis=0)
    left = [zero] * team
    left[1] = left[1] + ends[1]
    left[team - 1] = left[team - 1] + pltpu.roll(ends[team - 1], sweeps, 1)
    m_is = jnp.concatenate(left, axis=0)
    m_ss = jnp.concatenate([ends[0], pltpu.roll(ends[team], sweeps, 1)], axis=0)
    tt, ff = inverse(m_ii, sweeps, depth, seed(m_ii, depth), halves(m_is))
    msi_h = halves(m_si)
    ltp_ref[...] = packed(m_ss - exact(msi_h, halves(ff)), sweeps)
    @pl.when((member < team - 1) | (c < last))
    def _():
        pl.semaphore_wait(arrived, 1)

    for i, offset in enumerate(offsets):
        @pl.when(there(offset))
        def _():
            b_copy(i, 3 - i).start()
    tt_h = halves(tt)
    kk_h = halves(exact(msi_h, tt_h))
    for step in range(1, team):
        p_copy(step).wait_recv()
    sums = [jnp.zeros((sweeps, part), jnp.float32)]
    for j in range(1, team):
        sums.append(p_in[j - 1, sweeps:] + p_in[j, :sweeps])
    q_i = halves(jnp.concatenate(sums, axis=0))
    q_s = jnp.concatenate([p_in[0, :sweeps], p_in[team - 1, sweeps:]], axis=0)
    q = q_s - product(kk_h, q_i)
    for j in range(4):
        q_ref[j] = q[j * half:(j + 1) * half]
    q_ref[4] = q[:half]
    for i, offset in enumerate(offsets):
        @pl.when(there(offset))
        def _():
            q_copy(i, 3 - i).start()
    z_i = product(tt_h, q_i)
    for j in range(1, team):
        z_all[j] = z_i[j * sweeps:(j + 1) * sweeps]
    for step in range(1, team):
        z_copy(step).start()

    at_left = jnp.where(on_diagonal(zero.shape), 1.0, 0.0)
    follow[0] = at_left
    for j in range(1, team):
        follow[j] = -ff[j * sweeps:(j + 1) * sweeps]
    follow[team] = turn(at_left, sweeps)
    mine_h = halves(follow[pl.ds(member, 2)].reshape(edge, LANES))
    cf_h = halves(product(cm_h, mine_h)[:, :edge])
    cf3 = jnp.concatenate([cf_h[0], cf_h[1], cf_h[0]], axis=1)

    for i, offset in enumerate(offsets):
        @pl.when(there(offset))
        def _():
            b_copy(i, i).wait_recv()
    here = unpacked(ltp_ref[...], sweeps)
    near_l = unpacked(ltp_in[1], sweeps)
    near_r = unpacked(ltp_in[2], sweeps)
    far_l = unpacked(ltp_in[0], sweeps)[1]
    far_r = unpacked(ltp_in[3], sweeps)[0]
    big = jnp.concatenate([
        near_l[0] + turn(jnp.where(first, 0.0, far_l), -sweeps),
        near_l[1] + turn(here[0], sweeps),
        turn(here[1], sweeps) + turn(near_r[0], 2 * sweeps),
        turn(near_r[1], 2 * sweeps) + turn(jnp.where(first, far_r, 0.0), 3 * sweeps),
    ], axis=0)
    s_h = halves(inverse(big, sweeps, half // 2, seed(big, half // 2))[sweeps:3 * sweeps])

    for i, offset in enumerate(offsets):
        @pl.when(there(offset))
        def _():
            q_copy(i, i).wait_recv()
    none = jnp.zeros((half, part), jnp.float32)
    rhs = jnp.concatenate([
        far_in[0] + near_in[0, 2],
        none,
        near_in[0, 0] + q_ref[0],
        near_in[0, 1] + q_ref[1],
        q_ref[2] + near_in[1, 0],
        q_ref[3] + near_in[1, 1],
        near_in[1, 2] + far_in[1],
        none,
    ], axis=0)
    y_s = product(s_h, halves(rhs))
    y_in[member] = y_s
    for step in range(1, team):
        y_copy(step).start()

    cm3 = jnp.concatenate([cm_h[0], cm_h[1], cm_h[0]], axis=1)

    def apply(left, y):
        y_h = halves(y)
        y3 = jnp.concatenate([y_h[0], y_h[0], y_h[1]], axis=0)
        return lax.dot_general(left, y3, (((1,), (0,)), ((), ())), preferred_element_type=jnp.float32)

    z_in[member] = z_all[pl.ds(member, 2)]
    for step in range(1, team):
        z_copy(step).wait_recv()
    for j in range(team):
        cols = slice(j * part, (j + 1) * part)
        ax_ref[:, cols] = ax_ref[:, cols] - apply(cm3, z_in[j].reshape(edge, part))

    def last_step(j):
        cols = pl.ds(pl.multiple_of(j * part, part), part)
        out_ref[:, cols] = ax_ref[:, cols] - apply(cf3, y_in[j])

    last_step(member)
    for step in range(1, team):
        y_copy(step).wait_recv()
        last_step(mate(team - step))

    for copy in copies:
        copy.wait_send()
    for step in range(1, team):
        lt_copy(step).wait_send()
        p_copy(step).wait_send()
        y_copy(step).wait_send()
        z_copy(step).wait_send()
    for i, offset in enumerate(offsets):
        @pl.when(there(offset))
        def _():
            b_copy(i, 3 - i).wait_send()
            q_copy(i, 3 - i).wait_send()


def per_device(nrows, ncols, eigvecs, reflectors, starts):
    height, width = eigvecs.shape
    sweeps = starts.shape[0]
    team = sweeps // (2 * (height // BAND))
    part = width // team
    assert team * sweeps == LANES and nrows % team == 0
    f32 = jnp.float32
    hbm = pl.BlockSpec(memory_space=pltpu.HBM)
    dma = pltpu.SemaphoreType.DMA
    return pl.pallas_call(
        functools.partial(kernel, nrows, ncols),
        out_shape=jax.ShapeDtypeStruct((height, width), f32),
        in_specs=[hbm, hbm, hbm],
        out_specs=pl.BlockSpec(memory_space=pltpu.VMEM),
        scratch_shapes=[
            pltpu.VMEM((height, width), f32),
            pltpu.VMEM((sweeps, height), f32),
            pltpu.VMEM((1, sweeps), jnp.int32),
            pltpu.VMEM((team, sweeps, LANES), f32),
            pltpu.VMEM((team, 2 * sweeps, part), f32),
            pltpu.VMEM((team, 2 * sweeps, part), f32),
            pltpu.VMEM((sweeps, LANES), f32),
            pltpu.VMEM((4, sweeps, LANES), f32),
            pltpu.VMEM((team + 1, sweeps, LANES), f32),
            pltpu.VMEM((5, sweeps // 2, part), f32),
            pltpu.VMEM((2, 3, sweeps // 2, part), f32),
            pltpu.VMEM((2, sweeps // 2, part), f32),
            pltpu.VMEM((team + 1, sweeps, part), f32),
            pltpu.VMEM((team, 2, sweeps, part), f32),
            pltpu.VMEM((team, 2 * sweeps, part), f32),
            pltpu.VMEM((height, width), f32),
            dma, dma, dma,
            dma((ncols - 1,)), dma((ncols - 1,)),
            dma((team - 1,)), dma((team - 1,)),
            dma((team - 1,)), dma((team - 1,)),
            dma((4,)), dma((4,)),
            dma((4,)), dma((4,)),
            dma((team - 1,)), dma((team - 1,)),
            dma((team - 1,)), dma((team - 1,)),
            pltpu.SemaphoreType.REGULAR, pltpu.SemaphoreType.REGULAR, pltpu.SemaphoreType.REGULAR,
        ],
        compiler_params=pltpu.CompilerParams(
            collective_id=0, has_side_effects=True, vmem_limit_bytes=32 * 1024 * 1024),
    )(*(pltpu.with_memory_space_constraint(a, pltpu.HBM)
        for a in (eigvecs, reflectors, starts.reshape(1, sweeps))))


def solution(mesh):
    in_specs = (P("rows", "cols"), P("cols", "rows"), P())
    out_specs = P("rows", "cols")
    body = functools.partial(per_device, mesh.shape["rows"], mesh.shape["cols"])
    return jax.shard_map(
        body, mesh=mesh, in_specs=in_specs, out_specs=out_specs, check_vma=False
    )
```

```python
import functools
import jax
import jax.numpy as jnp
from jax import lax
from jax.experimental import pallas as pl
from jax.experimental.pallas import tpu as pltpu
from jax.sharding import PartitionSpec as P

BAND = 64
LANES = 128
MESH = pl.DeviceIdType.MESH


def halves(a):
    high = a.astype(jnp.bfloat16)
    return high, (a - high.astype(jnp.float32)).astype(jnp.bfloat16)


def product(a, b, ca=1, cb=0):
    def one(left, right):
        return lax.dot_general(
            left, right, (((ca,), (cb,)), ((), ())), preferred_element_type=jnp.float32)
    return one(a[0], b[0]) + (one(a[0], b[1]) + one(a[1], b[0]))


def exact(a, b):
    left = jnp.concatenate(a, axis=1)
    right = jnp.concatenate(b, axis=1)
    both = lax.dot_general(
        left, jnp.concatenate([right, right], axis=0), (((1,), (0,)), ((), ())),
        preferred_element_type=jnp.float32)
    width = both.shape[1] // 2
    return both[:, :width] + both[:, width:]


def gram(a, b):
    return product(a, b, 1, 1) + lax.dot_general(
        a[1], b[1], (((1,), (1,)), ((), ())), preferred_element_type=jnp.float32)


def packed(a, sweeps):
    return a[:sweeps] + pltpu.roll(a[sweeps:], 2 * sweeps, 1)


def turn(a, by):
    return pltpu.roll(a, by % LANES, 1) if by % LANES else a


def unpacked(a, sweeps, by=0):
    inside = (lanes_of(a) - by) % LANES < 2 * sweeps
    return [jnp.where(inside, turn(a, by + side * 2 * sweeps), 0.0) for side in range(2)]


def lanes_of(a):
    return lax.broadcasted_iota(jnp.int32, a.shape, 1)


def sweep_pair(shape, sweeps):
    rows = lax.broadcasted_iota(jnp.int32, shape, 0) % sweeps
    cols = lax.broadcasted_iota(jnp.int32, shape, 1) % sweeps
    return rows, cols


def lower(full, sweeps):
    rows, cols = sweep_pair(full.shape, sweeps)
    return jnp.where(rows > cols, full, 0.0)


def on_diagonal(shape):
    return lax.broadcasted_iota(jnp.int32, shape, 0) == lax.broadcasted_iota(jnp.int32, shape, 1)


def seed(full, size):
    lanes = full.shape[1]
    eye = on_diagonal(full.shape)
    diag = jnp.where(eye, full, 0.0)
    down = jnp.sum(diag, axis=1, keepdims=True)
    across = jnp.sum(diag, axis=0, keepdims=True)
    down = 1.0 / jnp.where(down == 0.0, 1.0, down)
    across = 1.0 / jnp.where(across == 0.0, 1.0, across)
    rows = lax.broadcasted_iota(jnp.int32, full.shape, 0)
    cols = lax.broadcasted_iota(jnp.int32, full.shape, 1)
    scaled = jnp.where((rows ^ cols) < size, down * full, 0.0)
    below = [jnp.where(rows - cols == m, scaled, 0.0) for m in range(size)]
    below = [jnp.sum(entries, axis=0, keepdims=True) for entries in below]
    terms = [across]
    for k in range(1, size):
        total = below[k] * across
        for m in range(1, k):
            total = total + pltpu.roll(below[m], lanes - (k - m), 1) * terms[k - m]
        terms.append(-total)
    done = jnp.where(eye, across, 0.0)
    for k in range(1, size):
        done = jnp.where(rows - cols == k, terms[k], done)
    return done


def seed_pairs(full, sweeps):
    eye = on_diagonal(full.shape)
    diag = jnp.where(eye, full, 0.0)
    down = jnp.sum(diag, axis=1, keepdims=True)
    across = jnp.sum(diag, axis=0, keepdims=True)
    down = 1.0 / jnp.where(down == 0.0, 1.0, down)
    across = 1.0 / jnp.where(across == 0.0, 1.0, across)
    rows, cols = sweep_pair(full.shape, sweeps)
    pair = ((rows ^ cols) == 1) & (rows > cols)
    return jnp.where(eye, down, 0.0) - down * jnp.where(pair, full, 0.0) * across


def inverse(full, sweeps, size, done, right=None):
    rows, cols = sweep_pair(full.shape, sweeps)
    apart = rows ^ cols
    while size < sweeps:
        reach = min(4 * size, sweeps)
        off = jnp.where((apart >= size) & (apart < reach) & (rows > cols), full, 0.0)
        inner = halves(done)
        step = halves(exact(inner, halves(off)))
        if reach == sweeps and right is not None:
            done = jnp.concatenate([done, exact(inner, right)], axis=1)
            inner = halves(done)
        first = done - exact(step, inner)
        if reach > 2 * size:
            twice = exact(step, step)
            first = first + exact(halves(twice), halves(first))
        done = first
        size = reach
    if right is None:
        return done
    return done[:, :full.shape[1]], done[:, full.shape[1]:]


def kernel(nrows, ncols, x_hbm, v_hbm, starts_hbm, out_ref, x_ref, v_all, starts_ref, lt_in, p_out,
           p_in, ltp_ref, ltp_in, follow, q_ref, near_in, far_in, z_all, z_in, y_in, ax_ref, x_sem, s_sem, v_local,
           v_send, v_recv, l_send, l_recv, p_send, p_recv, b_send, b_recv, q_send, q_recv, z_send, z_recv,
           y_send, y_recv, paired, entered, arrived):
    d, c = lax.axis_index("rows"), lax.axis_index("cols")
    own = v_hbm.shape[0]
    sweeps = v_all.shape[0]
    height, width = x_ref.shape
    depth = height // BAND
    chunks, team, _, lane = p_in.shape
    part = chunks * lane
    half = sweeps // 2
    group, member = d // team, d % team
    groups = nrows // team
    place = v_all.at[pl.ds(pl.multiple_of(c * own, own), own)]
    mine = pltpu.make_async_copy(v_hbm, place, v_local)
    mine.start()
    begins = pltpu.make_async_copy(starts_hbm, starts_ref, s_sem)
    begins.start()
    load = pltpu.make_async_copy(x_hbm, x_ref, x_sem)

    offsets = (-2, -1, 1, 2)

    def there(offset):
        return group + offset >= 0 if offset < 0 else group + offset < groups

    def mate(step):
        return (member + step) % team

    last = ncols - 1
    base = group * team
    barrier = pltpu.get_barrier_semaphore()

    def greet(sem, slab, core):
        pl.semaphore_signal(sem, inc=1, device_id=(slab, core), device_id_type=MESH)

    @pl.when(c > 0)
    def _():
        greet(barrier, d, 0)

    @pl.when((member < team - 1) | (c < last))
    def _():
        greet(barrier, base + team - 1, last)
    for offset in offsets:
        @pl.when(there(offset))
        def _():
            greet(barrier, base + offset * team, last)
    z_all[0] = jnp.zeros_like(z_all[0])
    z_all[team] = jnp.zeros_like(z_all[0])
    for i, offset in enumerate(offsets):
        @pl.when(jnp.logical_not(there(offset)))
        def _():
            ltp_in[i] = jnp.zeros_like(ltp_in[i])
            if abs(offset) == 1:
                near_in[:, i - 1] = jnp.zeros_like(near_in[:, 0])
            else:
                far_in[:, i // 3] = jnp.zeros_like(far_in[:, 0])
    load.start()

    @pl.when(c == 0)
    def _():
        pl.semaphore_wait(barrier, last)
        for core in range(1, ncols):
            greet(paired, d, core)

    @pl.when(c > 0)
    def _():
        pl.semaphore_wait(paired, 1)

    mine.wait()
    copies = []
    for step in range(1, ncols):
        copy = pltpu.make_async_remote_copy(
            src_ref=place, dst_ref=place, send_sem=v_send.at[step - 1], recv_sem=v_recv.at[step - 1],
            device_id=(d, (c + step) % ncols), device_id_type=MESH)
        copy.start()
        copies.append(copy)

    @pl.when((member == team - 1) & (c == last))
    def _():
        pl.semaphore_wait(barrier, ncols * team - 1)
        for slab in range(team):
            for core in range(ncols):
                if slab < team - 1 or core < last:
                    greet(entered, base + slab, core)

    begins.wait()
    across = jnp.broadcast_to(starts_ref[...], (sweeps, sweeps))
    begin = jnp.sum(jnp.where(on_diagonal(across.shape), across, 0), axis=1, keepdims=True)
    row = lax.broadcasted_iota(jnp.int32, v_all.shape, 1)
    window = (row - begin + BAND) // BAND
    outside = ((window == 0) & (d == 0)) | ((window == depth) & (d == nrows - 1) & (begin > 0))
    load.wait()
    x_halves = halves(x_ref[...])
    for copy in copies:
        copy.wait_recv()

    v = v_all[...]
    v = jnp.where(outside, 0.0, v)
    parts = [jnp.where(window == k, v, 0.0) for k in range(depth + 1)]
    u_s = jnp.concatenate([parts[0], parts[depth]], axis=0)
    u_i = jnp.concatenate(parts[1:depth], axis=0)
    inside = u_i.shape[0]
    edge = 2 * sweeps
    half_s = 0.5 * jnp.sum(u_s * u_s, axis=1, keepdims=True)
    half_i = 0.5 * jnp.sum(u_i * u_i, axis=1, keepdims=True)
    half_i = jnp.concatenate([half_i, jnp.zeros((LANES - inside, 1), jnp.float32)], axis=0)
    pad = jnp.zeros((LANES - edge, height), jnp.float32)
    us_h, ui_h = halves(u_s), halves(u_i)
    all_h = halves(jnp.concatenate(
        [u_i, jnp.zeros((LANES - inside, height), jnp.float32), u_s, pad], axis=0))
    g = gram(tuple(a[:LANES + edge] for a in all_h), all_h)
    g_ii, n_is = g[:LANES, :LANES], lower(g[:LANES, LANES:], sweeps)
    n_si, g_ss = lower(g[LANES:, :LANES], sweeps), g[LANES:, LANES:]
    l_ii = jnp.where(on_diagonal(g_ii.shape), half_i, lower(g_ii, sweeps))
    n_ss = jnp.where(on_diagonal(g_ss.shape), half_s, lower(g_ss, sweeps))
    wi_h = halves(product(ui_h, x_halves))
    w_s = product(us_h, x_halves)
    t, f = inverse(l_ii, sweeps, 2, seed_pairs(l_ii, sweeps), halves(n_is))
    nsi_h = halves(n_si)
    lt_in[member] = packed(n_ss - exact(nsi_h, halves(f)), sweeps)
    t_h = halves(t)
    k_h = tuple(a[:, :inside] for a in halves(exact(nsi_h, t_h)))
    t_h = tuple(a[:inside, :inside] for a in t_h)

    def to_mate(step, src, dst, send, recv):
        return pltpu.make_async_remote_copy(
            src_ref=src, dst_ref=dst, send_sem=send, recv_sem=recv,
            device_id=(base + mate(step), c), device_id_type=MESH)

    def lt_copy(step, core):
        return pltpu.make_async_remote_copy(
            src_ref=lt_in.at[member], dst_ref=lt_in.at[member], send_sem=l_send.at[step - 1, core],
            recv_sem=l_recv.at[step - 1], device_id=(base + mate(step), core), device_id_type=MESH)

    def p_copy(step, ch):
        return to_mate(step, p_out.at[ch, mate(step)], p_in.at[ch, member],
                       p_send.at[step - 1, ch], p_recv.at[step - 1, ch])

    def z_copy(step):
        return to_mate(step, z_all.at[pl.ds(mate(step), 2)], z_in.at[member],
                       z_send.at[step - 1], z_recv.at[step - 1])

    def y_copy(step, ch):
        return to_mate(step, y_in.at[ch, member], y_in.at[ch, member],
                       y_send.at[step - 1, ch], y_recv.at[step - 1, ch])

    def b_copy(i, slot, core):
        return pltpu.make_async_remote_copy(
            src_ref=ltp_ref.at[i // 2], dst_ref=ltp_in.at[slot], send_sem=b_send.at[i, core],
            recv_sem=b_recv.at[slot], device_id=(d + offsets[i] * team, core), device_id_type=MESH)

    def q_copy(i, slot, ch):
        if offsets[i] == -2:
            src, dst = q_ref.at[ch, 0], far_in.at[ch, 1]
        elif offsets[i] == -1:
            src, dst = q_ref.at[ch, pl.ds(0, 3)], near_in.at[ch, 1]
        elif offsets[i] == 1:
            src, dst = q_ref.at[ch, pl.ds(2, 3)], near_in.at[ch, 0]
        else:
            src, dst = q_ref.at[ch, 2], far_in.at[ch, 0]
        return pltpu.make_async_remote_copy(
            src_ref=src, dst_ref=dst, send_sem=q_send.at[i, ch], recv_sem=q_recv.at[slot, ch],
            device_id=(d + offsets[i] * team, c), device_id_type=MESH)

    @pl.when((member < team - 1) | (c < last))
    def _():
        pl.semaphore_wait(entered, 1)

    @pl.when(c == last)
    def _():
        for core in range(ncols):
            for step in range(1, team):
                lt_copy(step, core).start()

    for ch in range(chunks):
        cols = slice(ch * team * lane, (ch + 1) * team * lane)
        p = w_s[:, cols] - product(k_h, tuple(a[:, cols] for a in wi_h))
        for j in range(team):
            p_out[ch, j] = p[:, j * lane:(j + 1) * lane]
        for step in range(1, team):
            p_copy(step, ch).start()
        p_in[ch, member] = p_out[ch, member]

    peers = sum(there(offset).astype(jnp.int32) for offset in offsets)

    @pl.when((member == 0) & (c == last))
    def _():
        pl.semaphore_wait(barrier, peers * ncols * team)
        for slab in range(team):
            for core in range(ncols):
                if slab > 0 or core < last:
                    greet(arrived, base + slab, core)

    u_t = u_i.T
    ut_h = halves(u_t)
    inner = product(t_h, wi_h)
    ax_ref[...] = x_ref[...] - product(ut_h, halves(inner))
    cm_h = halves(u_s.T - product(ut_h, halves(f[:inside, :edge])))

    for step in range(1, team):
        lt_copy(step, 0).wait_recv()
    zero = jnp.zeros((sweeps, LANES), jnp.float32)
    blocks = [zero] * (team + 1)
    for j in range(team):
        for side, rows in enumerate(unpacked(lt_in[j], sweeps, j * sweeps)):
            blocks[j + side] = blocks[j + side] + rows
    first = lanes_of(blocks[0]) < sweeps
    keep = [jnp.where(first, 0.0, block) for block in blocks]
    ends = [jnp.where(first, block, 0.0) for block in blocks]
    m_ii = jnp.concatenate([zero] + keep[1:team], axis=0)
    m_si = jnp.concatenate([keep[0], keep[team]], axis=0)
    left = [zero] * team
    left[1] = left[1] + ends[1]
    left[team - 1] = left[team - 1] + pltpu.roll(ends[team - 1], sweeps, 1)
    m_is = jnp.concatenate(left, axis=0)
    m_ss = jnp.concatenate([ends[0], pltpu.roll(ends[team], sweeps, 1)], axis=0)
    tt, ff = inverse(m_ii, sweeps, depth, seed(m_ii, depth), halves(m_is))
    msi_h = halves(m_si)
    ltp = m_ss - exact(msi_h, halves(ff))
    at_l, at_r = ltp[:sweeps], ltp[sweeps:]
    early = lax.broadcasted_iota(jnp.int32, zero.shape, 0) < half
    beside = (lanes_of(zero) >= sweeps) & (lanes_of(zero) < sweeps + half)
    to_left = jnp.where(first, at_l, jnp.where(beside, jnp.where(early, at_r, at_l), 0.0))
    to_right = jnp.where(first, turn(at_r, -sweeps), jnp.where(
        beside, turn(jnp.where(early, at_l, at_r), sweeps), 0.0))
    for side, rows in enumerate((to_left, to_right)):
        ltp_ref[side] = rows[:half] + turn(rows[half:], edge)
    @pl.when((member > 0) | (c < last))
    def _():
        pl.semaphore_wait(arrived, 1)

    for i, offset in enumerate(offsets):
        @pl.when(there(offset) & (c == last))
        def _():
            for core in range(ncols):
                b_copy(i, 3 - i, core).start()
    tt_h = halves(tt)
    kk_h = halves(exact(msi_h, tt_h))
    sums = []
    for ch in range(chunks):
        for step in range(1, team):
            p_copy(step, ch).wait_recv()
        rows = [jnp.zeros((sweeps, lane), jnp.float32)]
        for j in range(1, team):
            rows.append(p_in[ch, j - 1, sweeps:] + p_in[ch, j, :sweeps])
        q_i = halves(jnp.concatenate(rows, axis=0))
        q_s = jnp.concatenate([p_in[ch, 0, :sweeps], p_in[ch, team - 1, sweeps:]], axis=0)
        q = q_s - product(kk_h, q_i)
        for j in range(4):
            q_ref[ch, j] = q[j * half:(j + 1) * half]
        q_ref[ch, 4] = q[:half]
        for i, offset in enumerate(offsets):
            @pl.when(there(offset))
            def _():
                q_copy(i, 3 - i, ch).start()
        sums.append(q_i)
    z_i = product(tt_h, tuple(jnp.concatenate(halfs, axis=1) for halfs in zip(*sums)))
    for j in range(1, team):
        z_all[j] = z_i[j * sweeps:(j + 1) * sweeps]
    for step in range(1, team):
        z_copy(step).start()
    at_left = jnp.where(on_diagonal(zero.shape), 1.0, 0.0)
    follow[0] = at_left
    for j in range(1, team):
        follow[j] = -ff[j * sweeps:(j + 1) * sweeps]
    follow[team] = turn(at_left, sweeps)
    mine_h = halves(follow[pl.ds(member, 2)].reshape(edge, LANES))
    cf_h = halves(product(cm_h, mine_h)[:, :edge])
    cf3 = jnp.concatenate([cf_h[0], cf_h[1], cf_h[0]], axis=1)

    for i, offset in enumerate(offsets):
        @pl.when(there(offset))
        def _():
            b_copy(i, i, 0).wait_recv()
    def at(rows, low, high):
        return jnp.where((lanes_of(rows) >= low) & (lanes_of(rows) < high), rows, 0.0)

    far_l, near_l, near_r, far_r = (ltp_in[i] for i in range(4))
    up, down = turn(near_l, sweeps), turn(near_l, -sweeps)
    late = jnp.zeros((half, LANES), jnp.float32)
    big = jnp.concatenate([
        at(far_l + down, 0, half),
        late,
        at(up, sweeps, 2 * sweeps),
        at(down, sweeps, 2 * sweeps) + at(up, 0, half),
        at(turn(near_r, 2 * sweeps), 2 * sweeps, 3 * sweeps),
        at(near_r, 2 * sweeps, 3 * sweeps + half),
        at(turn(near_r, 2 * sweeps) + turn(far_r, 3 * sweeps), 3 * sweeps, 3 * sweeps + half),
        late,
    ], axis=0)
    here = turn(ltp, sweeps)
    big = big + jnp.concatenate([zero, here, zero], axis=0)
    s_h = halves(inverse(big, sweeps, half // 2, seed(big, half // 2))[sweeps:3 * sweeps])

    none = jnp.zeros((half, lane), jnp.float32)
    for ch in range(chunks):
        for i, offset in enumerate(offsets):
            @pl.when(there(offset))
            def _():
                q_copy(i, i, ch).wait_recv()
        rhs = jnp.concatenate([
            far_in[ch, 0] + near_in[ch, 0, 2],
            none,
            near_in[ch, 0, 0] + q_ref[ch, 0],
            near_in[ch, 0, 1] + q_ref[ch, 1],
            q_ref[ch, 2] + near_in[ch, 1, 0],
            q_ref[ch, 3] + near_in[ch, 1, 1],
            near_in[ch, 1, 2] + far_in[ch, 1],
            none,
        ], axis=0)
        y_in[ch, member] = product(s_h, halves(rhs))
        for step in range(1, team):
            y_copy(step, ch).start()

    cm3 = jnp.concatenate([cm_h[0], cm_h[1], cm_h[0]], axis=1)

    def apply(left, y):
        y_h = halves(y)
        y3 = jnp.concatenate([y_h[0], y_h[0], y_h[1]], axis=0)
        return lax.dot_general(left, y3, (((1,), (0,)), ((), ())), preferred_element_type=jnp.float32)

    z_in[member] = z_all[pl.ds(member, 2)]
    for step in range(1, team):
        z_copy(step).wait_recv()
    span = team * lane
    for ch in range(chunks):
        z = jnp.concatenate(
            [z_in[j].reshape(edge, part)[:, ch * lane:(ch + 1) * lane] for j in range(team)], axis=1)
        cols = slice(ch * span, (ch + 1) * span)
        ax_ref[:, cols] = ax_ref[:, cols] - apply(cm3, z)

    for ch in range(chunks - 1):
        for step in range(1, team):
            y_copy(step, ch).wait_recv()
        cols = slice(ch * span, (ch + 1) * span)
        y = jnp.concatenate([y_in[ch, j] for j in range(team)], axis=1)
        out_ref[:, cols] = ax_ref[:, cols] - apply(cf3, y)

    def last_step(j):
        cols = pl.ds(pl.multiple_of(((chunks - 1) * team + j) * lane, lane), lane)
        out_ref[:, cols] = ax_ref[:, cols] - apply(cf3, y_in[chunks - 1, j])

    last_step(member)
    for step in range(1, team):
        y_copy(step, chunks - 1).wait_recv()
        last_step(mate(team - step))

    for copy in copies:
        copy.wait_send()
    for step in range(1, team):
        for ch in range(chunks):
            p_copy(step, ch).wait_send()
            y_copy(step, ch).wait_send()
        z_copy(step).wait_send()
    for i, offset in enumerate(offsets):
        @pl.when(there(offset))
        def _():
            for ch in range(chunks):
                q_copy(i, 3 - i, ch).wait_send()

    @pl.when(c == last)
    def _():
        for core in range(ncols):
            for step in range(1, team):
                lt_copy(step, core).wait_send()
            for i, offset in enumerate(offsets):
                @pl.when(there(offset))
                def _():
                    b_copy(i, 3 - i, core).wait_send()


def per_device(nrows, ncols, eigvecs, reflectors, starts):
    height, width = eigvecs.shape
    sweeps = starts.shape[0]
    team = sweeps // (2 * (height // BAND))
    part = width // team
    lane = LANES
    chunks = part // lane
    assert team * sweeps == LANES and nrows % team == 0
    f32 = jnp.float32
    hbm = pl.BlockSpec(memory_space=pltpu.HBM)
    dma = pltpu.SemaphoreType.DMA
    return pl.pallas_call(
        functools.partial(kernel, nrows, ncols),
        out_shape=jax.ShapeDtypeStruct((height, width), f32),
        in_specs=[hbm, hbm, hbm],
        out_specs=pl.BlockSpec(memory_space=pltpu.VMEM),
        scratch_shapes=[
            pltpu.VMEM((height, width), f32),
            pltpu.VMEM((sweeps, height), f32),
            pltpu.VMEM((1, sweeps), jnp.int32),
            pltpu.VMEM((team, sweeps, LANES), f32),
            pltpu.VMEM((chunks, team, 2 * sweeps, lane), f32),
            pltpu.VMEM((chunks, team, 2 * sweeps, lane), f32),
            pltpu.VMEM((2, sweeps // 2, LANES), f32),
            pltpu.VMEM((4, sweeps // 2, LANES), f32),
            pltpu.VMEM((team + 1, sweeps, LANES), f32),
            pltpu.VMEM((chunks, 5, sweeps // 2, lane), f32),
            pltpu.VMEM((chunks, 2, 3, sweeps // 2, lane), f32),
            pltpu.VMEM((chunks, 2, sweeps // 2, lane), f32),
            pltpu.VMEM((team + 1, sweeps, part), f32),
            pltpu.VMEM((team, 2, sweeps, part), f32),
            pltpu.VMEM((chunks, team, 2 * sweeps, lane), f32),
            pltpu.VMEM((height, width), f32),
            dma, dma, dma,
            dma((ncols - 1,)), dma((ncols - 1,)),
            dma((team - 1, ncols)), dma((team - 1,)),
            dma((team - 1, chunks)), dma((team - 1, chunks)),
            dma((4, ncols)), dma((4,)),
            dma((4, chunks)), dma((4, chunks)),
            dma((team - 1,)), dma((team - 1,)),
            dma((team - 1, chunks)), dma((team - 1, chunks)),
            pltpu.SemaphoreType.REGULAR, pltpu.SemaphoreType.REGULAR, pltpu.SemaphoreType.REGULAR,
        ],
        compiler_params=pltpu.CompilerParams(
            collective_id=0, has_side_effects=True, vmem_limit_bytes=32 * 1024 * 1024),
    )(*(pltpu.with_memory_space_constraint(a, pltpu.HBM)
        for a in (eigvecs, reflectors, starts.reshape(1, sweeps))))


def solution(mesh):
    in_specs = (P("rows", "cols"), P("cols", "rows"), P())
    out_specs = P("rows", "cols")
    body = functools.partial(per_device, mesh.shape["rows"], mesh.shape["cols"])
    return jax.shard_map(
        body, mesh=mesh, in_specs=in_specs, out_specs=out_specs, check_vma=False
    )
```

```python
import functools
import jax
import jax.numpy as jnp
from jax import lax
from jax.experimental import pallas as pl
from jax.experimental.pallas import tpu as pltpu
from jax.sharding import PartitionSpec as P

BAND = 64
LANES = 128
MESH = pl.DeviceIdType.MESH


def halves(a):
    high = a.astype(jnp.bfloat16)
    return high, (a - high.astype(jnp.float32)).astype(jnp.bfloat16)


def product(a, b, ca=1, cb=0):
    def one(left, right):
        return lax.dot_general(
            left, right, (((ca,), (cb,)), ((), ())), preferred_element_type=jnp.float32)
    return one(a[0], b[0]) + (one(a[0], b[1]) + one(a[1], b[0]))


def exact(a, b):
    left = jnp.concatenate(a, axis=1)
    right = jnp.concatenate(b, axis=1)
    both = lax.dot_general(
        left, jnp.concatenate([right, right], axis=0), (((1,), (0,)), ((), ())),
        preferred_element_type=jnp.float32)
    width = both.shape[1] // 2
    return both[:, :width] + both[:, width:]


def gram(a, b):
    return product(a, b, 1, 1) + lax.dot_general(
        a[1], b[1], (((1,), (1,)), ((), ())), preferred_element_type=jnp.float32)


def packed(a, sweeps):
    return a[:sweeps] + pltpu.roll(a[sweeps:], 2 * sweeps, 1)


def turn(a, by):
    return pltpu.roll(a, by % LANES, 1) if by % LANES else a


def unpacked(a, sweeps, by=0):
    inside = (lanes_of(a) - by) % LANES < 2 * sweeps
    return [jnp.where(inside, turn(a, by + side * 2 * sweeps), 0.0) for side in range(2)]


def lanes_of(a):
    return lax.broadcasted_iota(jnp.int32, a.shape, 1)


def sweep_pair(shape, sweeps):
    rows = lax.broadcasted_iota(jnp.int32, shape, 0) % sweeps
    cols = lax.broadcasted_iota(jnp.int32, shape, 1) % sweeps
    return rows, cols


def lower(full, sweeps):
    rows, cols = sweep_pair(full.shape, sweeps)
    return jnp.where(rows > cols, full, 0.0)


def on_diagonal(shape):
    return lax.broadcasted_iota(jnp.int32, shape, 0) == lax.broadcasted_iota(jnp.int32, shape, 1)


def seed(full, size):
    lanes = full.shape[1]
    eye = on_diagonal(full.shape)
    diag = jnp.where(eye, full, 0.0)
    down = jnp.sum(diag, axis=1, keepdims=True)
    across = jnp.sum(diag, axis=0, keepdims=True)
    down = 1.0 / jnp.where(down == 0.0, 1.0, down)
    across = 1.0 / jnp.where(across == 0.0, 1.0, across)
    rows = lax.broadcasted_iota(jnp.int32, full.shape, 0)
    cols = lax.broadcasted_iota(jnp.int32, full.shape, 1)
    scaled = jnp.where((rows ^ cols) < size, down * full, 0.0)
    below = [jnp.where(rows - cols == m, scaled, 0.0) for m in range(size)]
    below = [jnp.sum(entries, axis=0, keepdims=True) for entries in below]
    terms = [across]
    for k in range(1, size):
        total = below[k] * across
        for m in range(1, k):
            total = total + pltpu.roll(below[m], lanes - (k - m), 1) * terms[k - m]
        terms.append(-total)
    done = jnp.where(eye, across, 0.0)
    for k in range(1, size):
        done = jnp.where(rows - cols == k, terms[k], done)
    return done


def seed_pairs(full, sweeps):
    eye = on_diagonal(full.shape)
    diag = jnp.where(eye, full, 0.0)
    down = jnp.sum(diag, axis=1, keepdims=True)
    across = jnp.sum(diag, axis=0, keepdims=True)
    down = 1.0 / jnp.where(down == 0.0, 1.0, down)
    across = 1.0 / jnp.where(across == 0.0, 1.0, across)
    rows, cols = sweep_pair(full.shape, sweeps)
    pair = ((rows ^ cols) == 1) & (rows > cols)
    return jnp.where(eye, down, 0.0) - down * jnp.where(pair, full, 0.0) * across


def inverse(full, sweeps, size, done, right=None):
    rows, cols = sweep_pair(full.shape, sweeps)
    apart = rows ^ cols
    while size < sweeps:
        reach = min(4 * size, sweeps)
        off = jnp.where((apart >= size) & (apart < reach) & (rows > cols), full, 0.0)
        inner = halves(done)
        step = halves(exact(inner, halves(off)))
        if reach == sweeps and right is not None:
            done = jnp.concatenate([done, exact(inner, right)], axis=1)
            inner = halves(done)
        first = done - exact(step, inner)
        if reach > 2 * size:
            twice = exact(step, step)
            first = first + exact(halves(twice), halves(first))
        done = first
        size = reach
    if right is None:
        return done
    return done[:, :full.shape[1]], done[:, full.shape[1]:]


def kernel(nrows, ncols, x_hbm, v_hbm, starts_hbm, out_ref, x_ref, v_all, starts_ref, lt_in, p_out,
           p_in, ltp_ref, ltp_in, follow, q_ref, near_in, far_in, z_all, z_in, y_in, ax_ref, x_sem, s_sem, v_local,
           v_send, v_recv, l_send, l_recv, p_send, p_recv, b_send, b_recv, q_send, q_recv, z_send, z_recv,
           y_send, y_recv, paired, entered, arrived):
    d, c = lax.axis_index("rows"), lax.axis_index("cols")
    own = v_hbm.shape[0]
    sweeps = v_all.shape[0]
    height, width = x_ref.shape
    depth = height // BAND
    chunks, team, _, lane = p_in.shape
    part = chunks * lane
    half = sweeps // 2
    group, member = d // team, d % team
    groups = nrows // team
    place = v_all.at[pl.ds(pl.multiple_of(c * own, own), own)]
    mine = pltpu.make_async_copy(v_hbm, place, v_local)
    mine.start()
    begins = pltpu.make_async_copy(starts_hbm, starts_ref, s_sem)
    begins.start()
    load = pltpu.make_async_copy(x_hbm, x_ref, x_sem)

    offsets = (-2, -1, 1, 2)

    def there(offset):
        return group + offset >= 0 if offset < 0 else group + offset < groups

    def mate(step):
        return (member + step) % team

    last = ncols - 1
    base = group * team
    barrier = pltpu.get_barrier_semaphore()

    def greet(sem, slab, core):
        pl.semaphore_signal(sem, inc=1, device_id=(slab, core), device_id_type=MESH)

    @pl.when(c > 0)
    def _():
        greet(barrier, d, 0)

    @pl.when((member < team - 1) | (c < last))
    def _():
        greet(barrier, base + team - 1, last)
    for offset in offsets:
        @pl.when(there(offset))
        def _():
            greet(barrier, base + offset * team, last)
    z_all[:, 0] = jnp.zeros_like(z_all[:, 0])
    z_all[:, team] = jnp.zeros_like(z_all[:, 0])
    for i, offset in enumerate(offsets):
        @pl.when(jnp.logical_not(there(offset)))
        def _():
            ltp_in[i] = jnp.zeros_like(ltp_in[i])
            if abs(offset) == 1:
                near_in[:, i - 1] = jnp.zeros_like(near_in[:, 0])
            else:
                far_in[:, i // 3] = jnp.zeros_like(far_in[:, 0])
    load.start()

    @pl.when(c == 0)
    def _():
        pl.semaphore_wait(barrier, last)
        for core in range(1, ncols):
            greet(paired, d, core)

    @pl.when(c > 0)
    def _():
        pl.semaphore_wait(paired, 1)

    mine.wait()
    copies = []
    for step in range(1, ncols):
        copy = pltpu.make_async_remote_copy(
            src_ref=place, dst_ref=place, send_sem=v_send.at[step - 1], recv_sem=v_recv.at[step - 1],
            device_id=(d, (c + step) % ncols), device_id_type=MESH)
        copy.start()
        copies.append(copy)

    @pl.when((member == team - 1) & (c == last))
    def _():
        pl.semaphore_wait(barrier, ncols * team - 1)
        for slab in range(team):
            for core in range(ncols):
                if slab < team - 1 or core < last:
                    greet(entered, base + slab, core)

    begins.wait()
    across = jnp.broadcast_to(starts_ref[...], (sweeps, sweeps))
    begin = jnp.sum(jnp.where(on_diagonal(across.shape), across, 0), axis=1, keepdims=True)
    row = lax.broadcasted_iota(jnp.int32, v_all.shape, 1)
    window = (row - begin + BAND) // BAND
    outside = ((window == 0) & (d == 0)) | ((window == depth) & (d == nrows - 1) & (begin > 0))
    for copy in copies:
        copy.wait_recv()

    v = v_all[...]
    v = jnp.where(outside, 0.0, v)
    parts = [jnp.where(window == k, v, 0.0) for k in range(depth + 1)]
    u_s = jnp.concatenate([parts[0], parts[depth]], axis=0)
    u_i = jnp.concatenate(parts[1:depth], axis=0)
    inside = u_i.shape[0]
    edge = 2 * sweeps
    half_s = 0.5 * jnp.sum(u_s * u_s, axis=1, keepdims=True)
    half_i = 0.5 * jnp.sum(u_i * u_i, axis=1, keepdims=True)
    half_i = jnp.concatenate([half_i, jnp.zeros((LANES - inside, 1), jnp.float32)], axis=0)
    pad = jnp.zeros((LANES - edge, height), jnp.float32)
    us_h, ui_h = halves(u_s), halves(u_i)
    all_h = halves(jnp.concatenate(
        [u_i, jnp.zeros((LANES - inside, height), jnp.float32), u_s, pad], axis=0))
    g = gram(tuple(a[:LANES + edge] for a in all_h), all_h)
    g_ii, n_is = g[:LANES, :LANES], lower(g[:LANES, LANES:], sweeps)
    n_si, g_ss = lower(g[LANES:, :LANES], sweeps), g[LANES:, LANES:]
    l_ii = jnp.where(on_diagonal(g_ii.shape), half_i, lower(g_ii, sweeps))
    n_ss = jnp.where(on_diagonal(g_ss.shape), half_s, lower(g_ss, sweeps))
    t, f = inverse(l_ii, sweeps, 2, seed_pairs(l_ii, sweeps), halves(n_is))
    nsi_h = halves(n_si)
    lt_in[member] = packed(n_ss - exact(nsi_h, halves(f)), sweeps)
    t_h = halves(t)
    k_h = tuple(a[:, :inside] for a in halves(exact(nsi_h, t_h)))
    t_h = tuple(a[:inside, :inside] for a in t_h)

    def to_mate(step, src, dst, send, recv):
        return pltpu.make_async_remote_copy(
            src_ref=src, dst_ref=dst, send_sem=send, recv_sem=recv,
            device_id=(base + mate(step), c), device_id_type=MESH)

    def lt_copy(step, core):
        return pltpu.make_async_remote_copy(
            src_ref=lt_in.at[member], dst_ref=lt_in.at[member], send_sem=l_send.at[step - 1, core],
            recv_sem=l_recv.at[step - 1], device_id=(base + mate(step), core), device_id_type=MESH)

    def p_copy(step, ch):
        return to_mate(step, p_out.at[ch, mate(step)], p_in.at[ch, member],
                       p_send.at[step - 1, ch], p_recv.at[step - 1, ch])

    def z_copy(step, ch):
        return to_mate(step, z_all.at[ch, pl.ds(mate(step), 2)], z_in.at[ch, member],
                       z_send.at[step - 1, ch], z_recv.at[step - 1, ch])

    read = -(-(edge - depth * (team - 1)) // 8) * 8

    def reads(j):
        return depth * j // 8 * 8

    def y_copy(step, ch):
        rows = pl.ds(pl.multiple_of(reads(mate(step)), 8), read)
        return to_mate(step, y_in.at[ch, member, rows], y_in.at[ch, member, rows],
                       y_send.at[step - 1, ch], y_recv.at[step - 1, ch])

    def b_copy(i, slot, core):
        return pltpu.make_async_remote_copy(
            src_ref=ltp_ref.at[i // 2], dst_ref=ltp_in.at[slot], send_sem=b_send.at[i, core],
            recv_sem=b_recv.at[slot], device_id=(d + offsets[i] * team, core), device_id_type=MESH)

    def q_copy(i, slot, ch):
        if offsets[i] == -2:
            src, dst = q_ref.at[ch, 0], far_in.at[ch, 1]
        elif offsets[i] == -1:
            src, dst = q_ref.at[ch, pl.ds(0, 3)], near_in.at[ch, 1]
        elif offsets[i] == 1:
            src, dst = q_ref.at[ch, pl.ds(2, 3)], near_in.at[ch, 0]
        else:
            src, dst = q_ref.at[ch, 2], far_in.at[ch, 0]
        return pltpu.make_async_remote_copy(
            src_ref=src, dst_ref=dst, send_sem=q_send.at[i, ch], recv_sem=q_recv.at[slot, ch],
            device_id=(d + offsets[i] * team, c), device_id_type=MESH)

    @pl.when((member < team - 1) | (c < last))
    def _():
        pl.semaphore_wait(entered, 1)

    @pl.when(c == last)
    def _():
        for core in range(ncols):
            for step in range(1, team):
                lt_copy(step, core).start()

    load.wait()
    span = team * lane
    slices = [slice(ch * span, (ch + 1) * span) for ch in range(chunks)]
    wi_h = []
    for ch in range(chunks):
        x_h = halves(x_ref[:, slices[ch]])
        wi_h.append(halves(product(ui_h, x_h)))
        p = product(us_h, x_h) - product(k_h, wi_h[ch])
        for j in range(team):
            p_out[ch, j] = p[:, j * lane:(j + 1) * lane]
        for step in range(1, team):
            p_copy(step, ch).start()
        p_in[ch, member] = p_out[ch, member]

    peers = sum(there(offset).astype(jnp.int32) for offset in offsets)

    @pl.when((member == 0) & (c == last))
    def _():
        pl.semaphore_wait(barrier, peers * ncols * team)
        for slab in range(team):
            for core in range(ncols):
                if slab > 0 or core < last:
                    greet(arrived, base + slab, core)

    u_t = u_i.T
    ut_h = halves(u_t)
    for ch, cols in enumerate(slices):
        inner = product(t_h, wi_h[ch])
        ax_ref[:, cols] = x_ref[:, cols] - product(ut_h, halves(inner))
    cm_h = halves(u_s.T - product(ut_h, halves(f[:inside, :edge])))

    for step in range(1, team):
        lt_copy(step, 0).wait_recv()
    zero = jnp.zeros((sweeps, LANES), jnp.float32)
    blocks = [zero] * (team + 1)
    for j in range(team):
        for side, rows in enumerate(unpacked(lt_in[j], sweeps, j * sweeps)):
            blocks[j + side] = blocks[j + side] + rows
    first = lanes_of(blocks[0]) < sweeps
    keep = [jnp.where(first, 0.0, block) for block in blocks]
    ends = [jnp.where(first, block, 0.0) for block in blocks]
    m_ii = jnp.concatenate([zero] + keep[1:team], axis=0)
    m_si = jnp.concatenate([keep[0], keep[team]], axis=0)
    left = [zero] * team
    left[1] = left[1] + ends[1]
    left[team - 1] = left[team - 1] + pltpu.roll(ends[team - 1], sweeps, 1)
    m_is = jnp.concatenate(left, axis=0)
    m_ss = jnp.concatenate([ends[0], pltpu.roll(ends[team], sweeps, 1)], axis=0)
    tt, ff = inverse(m_ii, sweeps, depth, seed(m_ii, depth), halves(m_is))
    msi_h = halves(m_si)
    ltp = m_ss - exact(msi_h, halves(ff))
    at_l, at_r = ltp[:sweeps], ltp[sweeps:]
    early = lax.broadcasted_iota(jnp.int32, zero.shape, 0) < half
    beside = (lanes_of(zero) >= sweeps) & (lanes_of(zero) < sweeps + half)
    to_left = jnp.where(first, at_l, jnp.where(beside, jnp.where(early, at_r, at_l), 0.0))
    to_right = jnp.where(first, turn(at_r, -sweeps), jnp.where(
        beside, turn(jnp.where(early, at_l, at_r), sweeps), 0.0))
    for side, rows in enumerate((to_left, to_right)):
        ltp_ref[side] = rows[:half] + turn(rows[half:], edge)
    @pl.when((member > 0) | (c < last))
    def _():
        pl.semaphore_wait(arrived, 1)

    for i, offset in enumerate(offsets):
        @pl.when(there(offset) & (c == last))
        def _():
            for core in range(ncols):
                b_copy(i, 3 - i, core).start()
    tt_h = halves(tt)
    kk_h = halves(exact(msi_h, tt_h))
    for ch in range(chunks):
        for step in range(1, team):
            p_copy(step, ch).wait_recv()
        rows = [jnp.zeros((sweeps, lane), jnp.float32)]
        for j in range(1, team):
            rows.append(p_in[ch, j - 1, sweeps:] + p_in[ch, j, :sweeps])
        q_i = halves(jnp.concatenate(rows, axis=0))
        q_s = jnp.concatenate([p_in[ch, 0, :sweeps], p_in[ch, team - 1, sweeps:]], axis=0)
        q = q_s - product(kk_h, q_i)
        for j in range(4):
            q_ref[ch, j] = q[j * half:(j + 1) * half]
        q_ref[ch, 4] = q[:half]
        for i, offset in enumerate(offsets):
            @pl.when(there(offset))
            def _():
                q_copy(i, 3 - i, ch).start()
        z_i = product(tt_h, q_i)
        for j in range(1, team):
            z_all[ch, j] = z_i[j * sweeps:(j + 1) * sweeps]
        for step in range(1, team):
            z_copy(step, ch).start()
    new = lanes_of(m_ii)
    new = jnp.where(new < sweeps, sweeps - 8 - new + 2 * (new % 8), new)
    order = (lax.broadcasted_iota(jnp.int32, new.shape, 0) == new).astype(jnp.bfloat16)
    ff = sum(lax.dot_general(a, order, (((1,), (0,)), ((), ())), preferred_element_type=jnp.float32)
             for a in halves(ff))
    follow[0] = order[:sweeps].astype(jnp.float32)
    for j in range(1, team):
        follow[j] = -ff[j * sweeps:(j + 1) * sweeps]
    follow[team] = order[sweeps:edge].astype(jnp.float32)
    mine_h = halves(follow[pl.ds(member, 2)].reshape(edge, LANES))
    cf_h = halves(product(cm_h, mine_h)[:, :edge])
    cf3 = jnp.concatenate([cf_h[0], cf_h[1], cf_h[0]], axis=1)

    for i, offset in enumerate(offsets):
        @pl.when(there(offset))
        def _():
            b_copy(i, i, 0).wait_recv()
    def at(rows, low, high):
        return jnp.where((lanes_of(rows) >= low) & (lanes_of(rows) < high), rows, 0.0)

    far_l, near_l, near_r, far_r = (ltp_in[i] for i in range(4))
    up, down = turn(near_l, sweeps), turn(near_l, -sweeps)
    late = jnp.zeros((half, LANES), jnp.float32)
    big = jnp.concatenate([
        at(far_l + down, 0, half),
        late,
        at(up, sweeps, 2 * sweeps),
        at(down, sweeps, 2 * sweeps) + at(up, 0, half),
        at(turn(near_r, 2 * sweeps), 2 * sweeps, 3 * sweeps),
        at(near_r, 2 * sweeps, 3 * sweeps + half),
        at(turn(near_r, 2 * sweeps) + turn(far_r, 3 * sweeps), 3 * sweeps, 3 * sweeps + half),
        late,
    ], axis=0)
    here = turn(ltp, sweeps)
    big = big + jnp.concatenate([zero, here, zero], axis=0)
    full = inverse(big, sweeps, half // 2, seed(big, half // 2))[sweeps:3 * sweeps]
    s_h = halves(jnp.concatenate(
        [full[b:b + 8] for b in range(sweeps - 8, -1, -8)] + [full[sweeps:]], axis=0))

    none = jnp.zeros((half, lane), jnp.float32)
    for ch in range(chunks):
        for i, offset in enumerate(offsets):
            @pl.when(there(offset))
            def _():
                q_copy(i, i, ch).wait_recv()
        rhs = jnp.concatenate([
            far_in[ch, 0] + near_in[ch, 0, 2],
            none,
            near_in[ch, 0, 0] + q_ref[ch, 0],
            near_in[ch, 0, 1] + q_ref[ch, 1],
            q_ref[ch, 2] + near_in[ch, 1, 0],
            q_ref[ch, 3] + near_in[ch, 1, 1],
            near_in[ch, 1, 2] + far_in[ch, 1],
            none,
        ], axis=0)
        y_in[ch, member] = product(s_h, halves(rhs))
        for step in range(1, team):
            y_copy(step, ch).start()

    cm3 = jnp.concatenate([cm_h[0], cm_h[1], cm_h[0]], axis=1)

    def apply(left, y):
        y_h = halves(y)
        y3 = jnp.concatenate([y_h[0], y_h[0], y_h[1]], axis=0)
        return lax.dot_general(left, y3, (((1,), (0,)), ((), ())), preferred_element_type=jnp.float32)

    for ch in range(chunks):
        z_in[ch, member] = z_all[ch, pl.ds(member, 2)]
    for ch, cols in enumerate(slices):
        for step in range(1, team):
            z_copy(step, ch).wait_recv()
        z = jnp.concatenate([z_in[ch, j].reshape(edge, lane) for j in range(team)], axis=1)
        ax_ref[:, cols] = ax_ref[:, cols] - apply(cm3, z)

    row = lax.broadcasted_iota(jnp.int32, (edge, lane), 0)
    sent = (row >= reads(member)) & (row < reads(member) + read)

    for ch in range(chunks - 1):
        for step in range(1, team):
            y_copy(step, ch).wait_recv()
        cols = slices[ch]
        y = jnp.concatenate([jnp.where(sent, y_in[ch, j], 0.0) for j in range(team)], axis=1)
        out_ref[:, cols] = ax_ref[:, cols] - apply(cf3, y)

    def last_step(j):
        cols = pl.ds(pl.multiple_of(((chunks - 1) * team + j) * lane, lane), lane)
        out_ref[:, cols] = ax_ref[:, cols] - apply(cf3, jnp.where(sent, y_in[chunks - 1, j], 0.0))

    last_step(member)
    for step in range(1, team):
        y_copy(step, chunks - 1).wait_recv()
        last_step(mate(team - step))

    for copy in copies:
        copy.wait_send()
    for step in range(1, team):
        for ch in range(chunks):
            p_copy(step, ch).wait_send()
            z_copy(step, ch).wait_send()
            y_copy(step, ch).wait_send()
    for i, offset in enumerate(offsets):
        @pl.when(there(offset))
        def _():
            for ch in range(chunks):
                q_copy(i, 3 - i, ch).wait_send()

    @pl.when(c == last)
    def _():
        for core in range(ncols):
            for step in range(1, team):
                lt_copy(step, core).wait_send()
            for i, offset in enumerate(offsets):
                @pl.when(there(offset))
                def _():
                    b_copy(i, 3 - i, core).wait_send()


def per_device(nrows, ncols, eigvecs, reflectors, starts):
    height, width = eigvecs.shape
    sweeps = starts.shape[0]
    team = sweeps // (2 * (height // BAND))
    part = width // team
    lane = LANES
    chunks = part // lane
    assert team * sweeps == LANES and nrows % team == 0
    f32 = jnp.float32
    hbm = pl.BlockSpec(memory_space=pltpu.HBM)
    dma = pltpu.SemaphoreType.DMA
    return pl.pallas_call(
        functools.partial(kernel, nrows, ncols),
        out_shape=jax.ShapeDtypeStruct((height, width), f32),
        in_specs=[hbm, hbm, hbm],
        out_specs=pl.BlockSpec(memory_space=pltpu.VMEM),
        scratch_shapes=[
            pltpu.VMEM((height, width), f32),
            pltpu.VMEM((sweeps, height), f32),
            pltpu.VMEM((1, sweeps), jnp.int32),
            pltpu.VMEM((team, sweeps, LANES), f32),
            pltpu.VMEM((chunks, team, 2 * sweeps, lane), f32),
            pltpu.VMEM((chunks, team, 2 * sweeps, lane), f32),
            pltpu.VMEM((2, sweeps // 2, LANES), f32),
            pltpu.VMEM((4, sweeps // 2, LANES), f32),
            pltpu.VMEM((team + 1, sweeps, LANES), f32),
            pltpu.VMEM((chunks, 5, sweeps // 2, lane), f32),
            pltpu.VMEM((chunks, 2, 3, sweeps // 2, lane), f32),
            pltpu.VMEM((chunks, 2, sweeps // 2, lane), f32),
            pltpu.VMEM((chunks, team + 1, sweeps, lane), f32),
            pltpu.VMEM((chunks, team, 2, sweeps, lane), f32),
            pltpu.VMEM((chunks, team, 2 * sweeps, lane), f32),
            pltpu.VMEM((height, width), f32),
            dma, dma, dma,
            dma((ncols - 1,)), dma((ncols - 1,)),
            dma((team - 1, ncols)), dma((team - 1,)),
            dma((team - 1, chunks)), dma((team - 1, chunks)),
            dma((4, ncols)), dma((4,)),
            dma((4, chunks)), dma((4, chunks)),
            dma((team - 1, chunks)), dma((team - 1, chunks)),
            dma((team - 1, chunks)), dma((team - 1, chunks)),
            pltpu.SemaphoreType.REGULAR, pltpu.SemaphoreType.REGULAR, pltpu.SemaphoreType.REGULAR,
        ],
        compiler_params=pltpu.CompilerParams(
            collective_id=0, has_side_effects=True, vmem_limit_bytes=32 * 1024 * 1024),
    )(*(pltpu.with_memory_space_constraint(a, pltpu.HBM)
        for a in (eigvecs, reflectors, starts.reshape(1, sweeps))))


def solution(mesh):
    in_specs = (P("rows", "cols"), P("cols", "rows"), P())
    out_specs = P("rows", "cols")
    body = functools.partial(per_device, mesh.shape["rows"], mesh.shape["cols"])
    return jax.shard_map(
        body, mesh=mesh, in_specs=in_specs, out_specs=out_specs, check_vma=False
    )
```

```python
import functools
import jax
import jax.numpy as jnp
from jax import lax
from jax.experimental import pallas as pl
from jax.experimental.pallas import tpu as pltpu
from jax.sharding import PartitionSpec as P

BAND = 64
LANES = 128
MESH = pl.DeviceIdType.MESH


def halves(a):
    high = a.astype(jnp.bfloat16)
    return high, (a - high.astype(jnp.float32)).astype(jnp.bfloat16)


def product(a, b, ca=1, cb=0):
    def one(left, right):
        return lax.dot_general(
            left, right, (((ca,), (cb,)), ((), ())), preferred_element_type=jnp.float32)
    return one(a[0], b[0]) + (one(a[0], b[1]) + one(a[1], b[0]))


def exact(a, b):
    left = jnp.concatenate(a, axis=1)
    right = jnp.concatenate(b, axis=1)
    both = lax.dot_general(
        left, jnp.concatenate([right, right], axis=0), (((1,), (0,)), ((), ())),
        preferred_element_type=jnp.float32)
    width = both.shape[1] // 2
    return both[:, :width] + both[:, width:]


def gram(a, b):
    return product(a, b, 1, 1) + lax.dot_general(
        a[1], b[1], (((1,), (1,)), ((), ())), preferred_element_type=jnp.float32)


def packed(a, sweeps):
    return a[:sweeps] + pltpu.roll(a[sweeps:], 2 * sweeps, 1)


def turn(a, by):
    return pltpu.roll(a, by % LANES, 1) if by % LANES else a


def unpacked(a, sweeps, by=0):
    inside = (lanes_of(a) - by) % LANES < 2 * sweeps
    return [jnp.where(inside, turn(a, by + side * 2 * sweeps), 0.0) for side in range(2)]


def lanes_of(a):
    return lax.broadcasted_iota(jnp.int32, a.shape, 1)


def sweep_pair(shape, sweeps):
    rows = lax.broadcasted_iota(jnp.int32, shape, 0) % sweeps
    cols = lax.broadcasted_iota(jnp.int32, shape, 1) % sweeps
    return rows, cols


def lower(full, sweeps):
    rows, cols = sweep_pair(full.shape, sweeps)
    return jnp.where(rows > cols, full, 0.0)


def on_diagonal(shape):
    return lax.broadcasted_iota(jnp.int32, shape, 0) == lax.broadcasted_iota(jnp.int32, shape, 1)


def seed(full, size):
    lanes = full.shape[1]
    rows = lax.broadcasted_iota(jnp.int32, full.shape, 0)
    cols = lax.broadcasted_iota(jnp.int32, full.shape, 1)
    own = jnp.where((rows ^ cols) < size, full, 0.0)
    below = [jnp.sum(jnp.where(rows - cols == m, own, 0.0), axis=0, keepdims=True)
             for m in range(size)]
    across = 1.0 / jnp.where(below[0] == 0.0, 1.0, below[0])

    def ahead(a, by):
        return pltpu.roll(a, lanes - by, 1) if by else a

    terms = [across]
    for k in range(1, size):
        total = sum(ahead(below[m], k - m) * terms[k - m] for m in range(1, k + 1))
        terms.append(-ahead(across, k) * total)
    done = jnp.where(rows == cols, across, 0.0)
    for k in range(1, size):
        done = jnp.where(rows - cols == k, terms[k], done)
    return done


def seed_pairs(full, sweeps, diag):
    eye = on_diagonal(full.shape)
    down = 1.0 / jnp.where(diag == 0.0, 1.0, diag)
    across = jnp.sum(jnp.where(eye, down, 0.0), axis=0, keepdims=True)
    rows, cols = sweep_pair(full.shape, sweeps)
    pair = ((rows ^ cols) == 1) & (rows > cols)
    return jnp.where(eye, down, 0.0) - down * jnp.where(pair, full, 0.0) * across


def inverse(full, sweeps, size, done, right=None):
    rows, cols = sweep_pair(full.shape, sweeps)
    apart = rows ^ cols
    while size < sweeps:
        reach = min(4 * size, sweeps)
        off = jnp.where((apart >= size) & (apart < reach) & (rows > cols), full, 0.0)
        inner = halves(done)
        step = halves(exact(inner, halves(off)))
        if reach == sweeps and right is not None:
            done = jnp.concatenate([done, exact(inner, right)], axis=1)
            inner = halves(done)
        first = done - exact(step, inner)
        if reach > 2 * size:
            twice = exact(step, step)
            first = first + exact(halves(twice), halves(first))
        done = first
        size = reach
    if right is None:
        return done
    return done[:, :full.shape[1]], done[:, full.shape[1]:]


def kernel(nrows, ncols, x_hbm, v_hbm, starts_hbm, out_ref, x_ref, v_all, starts_ref, lt_in, p_out,
           p_in, ltp_ref, ltp_in, follow, q_ref, near_in, far_in, z_all, z_in, y_in, ax_ref, x_sem, s_sem, v_local,
           v_send, v_recv, l_send, l_recv, p_send, p_recv, b_send, b_recv, q_send, q_recv, z_send, z_recv,
           y_send, y_recv, paired, entered, arrived):
    d, c = lax.axis_index("rows"), lax.axis_index("cols")
    own = v_hbm.shape[0]
    sweeps = v_all.shape[0]
    height, width = x_ref.shape
    depth = height // BAND
    chunks, team, _, lane = p_in.shape
    part = chunks * lane
    half = sweeps // 2
    group, member = d // team, d % team
    groups = nrows // team
    place = v_all.at[pl.ds(pl.multiple_of(c * own, own), own)]
    mine = pltpu.make_async_copy(v_hbm, place, v_local)
    mine.start()
    begins = pltpu.make_async_copy(starts_hbm, starts_ref, s_sem)
    begins.start()
    load = pltpu.make_async_copy(x_hbm, x_ref, x_sem)

    offsets = (-2, -1, 1, 2)

    def there(offset):
        return group + offset >= 0 if offset < 0 else group + offset < groups

    def mate(step):
        return (member + step) % team

    last = ncols - 1
    base = group * team
    barrier = pltpu.get_barrier_semaphore()

    def greet(sem, slab, core):
        pl.semaphore_signal(sem, inc=1, device_id=(slab, core), device_id_type=MESH)

    @pl.when(c > 0)
    def _():
        greet(barrier, d, 0)

    @pl.when((member < team - 1) | (c < last))
    def _():
        greet(barrier, base + team - 1, last)
    for offset in offsets:
        @pl.when(there(offset))
        def _():
            greet(barrier, base + offset * team, last)
    z_all[:, 0] = jnp.zeros_like(z_all[:, 0])
    z_all[:, team] = jnp.zeros_like(z_all[:, 0])
    for i, offset in enumerate(offsets):
        @pl.when(jnp.logical_not(there(offset)))
        def _():
            ltp_in[i] = jnp.zeros_like(ltp_in[i])
            if abs(offset) == 1:
                near_in[:, i - 1] = jnp.zeros_like(near_in[:, 0])
            else:
                far_in[:, i // 3] = jnp.zeros_like(far_in[:, 0])
    load.start()

    @pl.when(c == 0)
    def _():
        pl.semaphore_wait(barrier, last)
        for core in range(1, ncols):
            greet(paired, d, core)

    @pl.when(c > 0)
    def _():
        pl.semaphore_wait(paired, 1)

    mine.wait()
    copies = []
    for step in range(1, ncols):
        copy = pltpu.make_async_remote_copy(
            src_ref=place, dst_ref=place, send_sem=v_send.at[step - 1], recv_sem=v_recv.at[step - 1],
            device_id=(d, (c + step) % ncols), device_id_type=MESH)
        copy.start()
        copies.append(copy)

    @pl.when((member == team - 1) & (c == last))
    def _():
        pl.semaphore_wait(barrier, ncols * team - 1)
        for slab in range(team):
            for core in range(ncols):
                if slab < team - 1 or core < last:
                    greet(entered, base + slab, core)

    begins.wait()
    across = jnp.broadcast_to(starts_ref[...], (sweeps, sweeps))
    begin = jnp.sum(jnp.where(on_diagonal(across.shape), across, 0), axis=1, keepdims=True)
    row = lax.broadcasted_iota(jnp.int32, v_all.shape, 1)
    window = (row - begin + BAND) // BAND
    outside = ((window == 0) & (d == 0)) | ((window == depth) & (d == nrows - 1) & (begin > 0))
    for copy in copies:
        copy.wait_recv()

    v = v_all[...]
    v = jnp.where(outside, 0.0, v)
    parts = [jnp.where(window == k, v, 0.0) for k in range(depth + 1)]
    u_s = jnp.concatenate([parts[0], parts[depth]], axis=0)
    u_i = jnp.concatenate(parts[1:depth], axis=0)
    inside = u_i.shape[0]
    edge = 2 * sweeps
    half_s = 0.5 * jnp.sum(u_s * u_s, axis=1, keepdims=True)
    half_i = 0.5 * jnp.sum(u_i * u_i, axis=1, keepdims=True)
    half_i = jnp.concatenate([half_i, jnp.zeros((LANES - inside, 1), jnp.float32)], axis=0)
    pad = jnp.zeros((LANES - edge, height), jnp.float32)
    us_h, ui_h = halves(u_s), halves(u_i)
    all_h = halves(jnp.concatenate(
        [u_i, jnp.zeros((LANES - inside, height), jnp.float32), u_s, pad], axis=0))
    g = gram(tuple(a[:LANES + edge] for a in all_h), all_h)
    g_ii, n_is = g[:LANES, :LANES], lower(g[:LANES, LANES:], sweeps)
    n_si, g_ss = lower(g[LANES:, :LANES], sweeps), g[LANES:, LANES:]
    l_ii = jnp.where(on_diagonal(g_ii.shape), half_i, lower(g_ii, sweeps))
    n_ss = jnp.where(on_diagonal(g_ss.shape), half_s, lower(g_ss, sweeps))
    t, f = inverse(l_ii, sweeps, 2, seed_pairs(l_ii, sweeps, half_i), halves(n_is))
    nsi_h = halves(n_si)
    lt_in[member] = packed(n_ss - exact(nsi_h, halves(f)), sweeps)
    t_h = halves(t)
    k_h = tuple(a[:, :inside] for a in halves(exact(nsi_h, t_h)))
    t_h = tuple(a[:inside, :inside] for a in t_h)

    def to_mate(step, src, dst, send, recv):
        return pltpu.make_async_remote_copy(
            src_ref=src, dst_ref=dst, send_sem=send, recv_sem=recv,
            device_id=(base + mate(step), c), device_id_type=MESH)

    def lt_copy(step, core):
        return pltpu.make_async_remote_copy(
            src_ref=lt_in.at[member], dst_ref=lt_in.at[member], send_sem=l_send.at[step - 1, core],
            recv_sem=l_recv.at[step - 1], device_id=(base + mate(step), core), device_id_type=MESH)

    def p_copy(step, ch):
        return to_mate(step, p_out.at[ch, mate(step)], p_in.at[ch, member],
                       p_send.at[step - 1, ch], p_recv.at[step - 1, ch])

    def z_copy(step, ch):
        return to_mate(step, z_all.at[ch, pl.ds(mate(step), 2)], z_in.at[ch, member],
                       z_send.at[step - 1, ch], z_recv.at[step - 1, ch])

    read = -(-(edge - depth * (team - 1)) // 8) * 8

    def reads(j):
        return depth * j // 8 * 8

    def y_copy(step, ch):
        rows = pl.ds(pl.multiple_of(reads(mate(step)), 8), read)
        return to_mate(step, y_in.at[ch, member, rows], y_in.at[ch, member, rows],
                       y_send.at[step - 1, ch], y_recv.at[step - 1, ch])

    def b_copy(i, slot, core):
        return pltpu.make_async_remote_copy(
            src_ref=ltp_ref.at[i // 2], dst_ref=ltp_in.at[slot], send_sem=b_send.at[i, core],
            recv_sem=b_recv.at[slot], device_id=(d + offsets[i] * team, core), device_id_type=MESH)

    def q_copy(i, slot, ch):
        if offsets[i] == -2:
            src, dst = q_ref.at[ch, 0], far_in.at[ch, 1]
        elif offsets[i] == -1:
            src, dst = q_ref.at[ch, pl.ds(0, 3)], near_in.at[ch, 1]
        elif offsets[i] == 1:
            src, dst = q_ref.at[ch, pl.ds(2, 3)], near_in.at[ch, 0]
        else:
            src, dst = q_ref.at[ch, 2], far_in.at[ch, 0]
        return pltpu.make_async_remote_copy(
            src_ref=src, dst_ref=dst, send_sem=q_send.at[i, ch], recv_sem=q_recv.at[slot, ch],
            device_id=(d + offsets[i] * team, c), device_id_type=MESH)

    @pl.when((member < team - 1) | (c < last))
    def _():
        pl.semaphore_wait(entered, 1)

    @pl.when(c == last)
    def _():
        for core in range(ncols):
            for step in range(1, team):
                lt_copy(step, core).start()

    load.wait()
    span = team * lane
    slices = [slice(ch * span, (ch + 1) * span) for ch in range(chunks)]
    wi_h = []
    for ch in range(chunks):
        x_h = halves(x_ref[:, slices[ch]])
        wi_h.append(halves(product(ui_h, x_h)))
        p = product(us_h, x_h) - product(k_h, wi_h[ch])
        for j in range(team):
            p_out[ch, j] = p[:, j * lane:(j + 1) * lane]
        for step in range(1, team):
            p_copy(step, ch).start()
        p_in[ch, member] = p_out[ch, member]

    peers = sum(there(offset).astype(jnp.int32) for offset in offsets)

    @pl.when((member == 0) & (c == last))
    def _():
        pl.semaphore_wait(barrier, peers * ncols * team)
        for slab in range(team):
            for core in range(ncols):
                if slab > 0 or core < last:
                    greet(arrived, base + slab, core)

    u_t = u_i.T
    ut_h = halves(u_t)
    for ch, cols in enumerate(slices):
        inner = product(t_h, wi_h[ch])
        ax_ref[:, cols] = x_ref[:, cols] - product(ut_h, halves(inner))
    cm_h = halves(u_s.T - product(ut_h, halves(f[:inside, :edge])))

    for step in range(1, team):
        lt_copy(step, 0).wait_recv()
    zero = jnp.zeros((sweeps, LANES), jnp.float32)
    blocks = [zero] * (team + 1)
    for j in range(team):
        for side, rows in enumerate(unpacked(lt_in[j], sweeps, j * sweeps)):
            blocks[j + side] = blocks[j + side] + rows
    first = lanes_of(blocks[0]) < sweeps
    keep = [jnp.where(first, 0.0, block) for block in blocks]
    ends = [jnp.where(first, block, 0.0) for block in blocks]
    m_ii = jnp.concatenate([zero] + keep[1:team], axis=0)
    m_si = jnp.concatenate([keep[0], keep[team]], axis=0)
    left = [zero] * team
    left[1] = left[1] + ends[1]
    left[team - 1] = left[team - 1] + pltpu.roll(ends[team - 1], sweeps, 1)
    m_is = jnp.concatenate(left, axis=0)
    m_ss = jnp.concatenate([ends[0], pltpu.roll(ends[team], sweeps, 1)], axis=0)
    tt, ff = inverse(m_ii, sweeps, depth, seed(m_ii, depth), halves(m_is))
    msi_h = halves(m_si)
    ltp = m_ss - exact(msi_h, halves(ff))
    at_l, at_r = ltp[:sweeps], ltp[sweeps:]
    early = lax.broadcasted_iota(jnp.int32, zero.shape, 0) < half
    beside = (lanes_of(zero) >= sweeps) & (lanes_of(zero) < sweeps + half)
    to_left = jnp.where(first, at_l, jnp.where(beside, jnp.where(early, at_r, at_l), 0.0))
    to_right = jnp.where(first, turn(at_r, -sweeps), jnp.where(
        beside, turn(jnp.where(early, at_l, at_r), sweeps), 0.0))
    for side, rows in enumerate((to_left, to_right)):
        ltp_ref[side] = rows[:half] + turn(rows[half:], edge)
    @pl.when((member > 0) | (c < last))
    def _():
        pl.semaphore_wait(arrived, 1)

    for i, offset in enumerate(offsets):
        @pl.when(there(offset) & (c == last))
        def _():
            for core in range(ncols):
                b_copy(i, 3 - i, core).start()
    tt_h = halves(tt)
    kk_h = halves(exact(msi_h, tt_h))
    for ch in range(chunks):
        for step in range(1, team):
            p_copy(step, ch).wait_recv()
        rows = [jnp.zeros((sweeps, lane), jnp.float32)]
        for j in range(1, team):
            rows.append(p_in[ch, j - 1, sweeps:] + p_in[ch, j, :sweeps])
        q_i = halves(jnp.concatenate(rows, axis=0))
        q_s = jnp.concatenate([p_in[ch, 0, :sweeps], p_in[ch, team - 1, sweeps:]], axis=0)
        q = q_s - product(kk_h, q_i)
        for j in range(4):
            q_ref[ch, j] = q[j * half:(j + 1) * half]
        q_ref[ch, 4] = q[:half]
        for i, offset in enumerate(offsets):
            @pl.when(there(offset))
            def _():
                q_copy(i, 3 - i, ch).start()
        z_i = product(tt_h, q_i)
        for j in range(1, team):
            z_all[ch, j] = z_i[j * sweeps:(j + 1) * sweeps]
        for step in range(1, team):
            z_copy(step, ch).start()
    new = lanes_of(m_ii)
    new = jnp.where(new < sweeps, sweeps - 8 - new + 2 * (new % 8), new)
    order = (lax.broadcasted_iota(jnp.int32, new.shape, 0) == new).astype(jnp.bfloat16)
    ff = sum(lax.dot_general(a, order, (((1,), (0,)), ((), ())), preferred_element_type=jnp.float32)
             for a in halves(ff))
    follow[0] = order[:sweeps].astype(jnp.float32)
    for j in range(1, team):
        follow[j] = -ff[j * sweeps:(j + 1) * sweeps]
    follow[team] = order[sweeps:edge].astype(jnp.float32)
    mine_h = halves(follow[pl.ds(member, 2)].reshape(edge, LANES))
    cf_h = halves(product(cm_h, mine_h)[:, :edge])
    cf3 = jnp.concatenate([cf_h[0], cf_h[1], cf_h[0]], axis=1)

    for i, offset in enumerate(offsets):
        @pl.when(there(offset))
        def _():
            b_copy(i, i, 0).wait_recv()
    def at(rows, low, high):
        return jnp.where((lanes_of(rows) >= low) & (lanes_of(rows) < high), rows, 0.0)

    far_l, near_l, near_r, far_r = (ltp_in[i] for i in range(4))
    up, down = turn(near_l, sweeps), turn(near_l, -sweeps)
    late = jnp.zeros((half, LANES), jnp.float32)
    big = jnp.concatenate([
        at(far_l + down, 0, half),
        late,
        at(up, sweeps, 2 * sweeps),
        at(down, sweeps, 2 * sweeps) + at(up, 0, half),
        at(turn(near_r, 2 * sweeps), 2 * sweeps, 3 * sweeps),
        at(near_r, 2 * sweeps, 3 * sweeps + half),
        at(turn(near_r, 2 * sweeps) + turn(far_r, 3 * sweeps), 3 * sweeps, 3 * sweeps + half),
        late,
    ], axis=0)
    here = turn(ltp, sweeps)
    big = big + jnp.concatenate([zero, here, zero], axis=0)
    def own_rows(a):
        blocks = [a[b:b + 8] for b in range(2 * sweeps - 8, sweeps - 1, -8)]
        return jnp.concatenate(blocks + [a[2 * sweeps:3 * sweeps]], axis=0)

    apart = [axis & (sweeps - 1) for axis in (
        lax.broadcasted_iota(jnp.int32, big.shape, 0), lax.broadcasted_iota(jnp.int32, big.shape, 1))]
    off = jnp.where((apart[0] >= half) & (apart[1] < half), big, 0.0)
    done = seed(big, half)
    near = own_rows(done)
    step = exact(halves(near), halves(off))
    s_h = halves(near - exact(halves(step), halves(done)))

    none = jnp.zeros((half, lane), jnp.float32)
    for ch in range(chunks):
        for i, offset in enumerate(offsets):
            @pl.when(there(offset))
            def _():
                q_copy(i, i, ch).wait_recv()
        rhs = jnp.concatenate([
            far_in[ch, 0] + near_in[ch, 0, 2],
            none,
            near_in[ch, 0, 0] + q_ref[ch, 0],
            near_in[ch, 0, 1] + q_ref[ch, 1],
            q_ref[ch, 2] + near_in[ch, 1, 0],
            q_ref[ch, 3] + near_in[ch, 1, 1],
            near_in[ch, 1, 2] + far_in[ch, 1],
            none,
        ], axis=0)
        y_in[ch, member] = product(s_h, halves(rhs))
        for step in range(1, team):
            y_copy(step, ch).start()

    cm3 = jnp.concatenate([cm_h[0], cm_h[1], cm_h[0]], axis=1)

    def apply(left, y):
        y_h = halves(y)
        y3 = jnp.concatenate([y_h[0], y_h[0], y_h[1]], axis=0)
        return lax.dot_general(left, y3, (((1,), (0,)), ((), ())), preferred_element_type=jnp.float32)

    for ch in range(chunks):
        z_in[ch, member] = z_all[ch, pl.ds(member, 2)]
    for ch, cols in enumerate(slices):
        for step in range(1, team):
            z_copy(step, ch).wait_recv()
        z = jnp.concatenate([z_in[ch, j].reshape(edge, lane) for j in range(team)], axis=1)
        ax_ref[:, cols] = ax_ref[:, cols] - apply(cm3, z)

    row = lax.broadcasted_iota(jnp.int32, (edge, lane), 0)
    sent = (row >= reads(member)) & (row < reads(member) + read)

    for ch in range(chunks - 1):
        for step in range(1, team):
            y_copy(step, ch).wait_recv()
        cols = slices[ch]
        y = jnp.concatenate([jnp.where(sent, y_in[ch, j], 0.0) for j in range(team)], axis=1)
        out_ref[:, cols] = ax_ref[:, cols] - apply(cf3, y)

    def last_step(j):
        cols = pl.ds(pl.multiple_of(((chunks - 1) * team + j) * lane, lane), lane)
        out_ref[:, cols] = ax_ref[:, cols] - apply(cf3, jnp.where(sent, y_in[chunks - 1, j], 0.0))

    last_step(member)
    for step in range(1, team):
        y_copy(step, chunks - 1).wait_recv()
        last_step(mate(team - step))

    for copy in copies:
        copy.wait_send()
    for step in range(1, team):
        for ch in range(chunks):
            p_copy(step, ch).wait_send()
            z_copy(step, ch).wait_send()
            y_copy(step, ch).wait_send()
    for i, offset in enumerate(offsets):
        @pl.when(there(offset))
        def _():
            for ch in range(chunks):
                q_copy(i, 3 - i, ch).wait_send()

    @pl.when(c == last)
    def _():
        for core in range(ncols):
            for step in range(1, team):
                lt_copy(step, core).wait_send()
            for i, offset in enumerate(offsets):
                @pl.when(there(offset))
                def _():
                    b_copy(i, 3 - i, core).wait_send()


def per_device(nrows, ncols, eigvecs, reflectors, starts):
    height, width = eigvecs.shape
    sweeps = starts.shape[0]
    team = sweeps // (2 * (height // BAND))
    part = width // team
    lane = LANES
    chunks = part // lane
    assert team * sweeps == LANES and nrows % team == 0
    f32 = jnp.float32
    hbm = pl.BlockSpec(memory_space=pltpu.HBM)
    dma = pltpu.SemaphoreType.DMA
    return pl.pallas_call(
        functools.partial(kernel, nrows, ncols),
        out_shape=jax.ShapeDtypeStruct((height, width), f32),
        in_specs=[hbm, hbm, hbm],
        out_specs=pl.BlockSpec(memory_space=pltpu.VMEM),
        scratch_shapes=[
            pltpu.VMEM((height, width), f32),
            pltpu.VMEM((sweeps, height), f32),
            pltpu.VMEM((1, sweeps), jnp.int32),
            pltpu.VMEM((team, sweeps, LANES), f32),
            pltpu.VMEM((chunks, team, 2 * sweeps, lane), f32),
            pltpu.VMEM((chunks, team, 2 * sweeps, lane), f32),
            pltpu.VMEM((2, sweeps // 2, LANES), f32),
            pltpu.VMEM((4, sweeps // 2, LANES), f32),
            pltpu.VMEM((team + 1, sweeps, LANES), f32),
            pltpu.VMEM((chunks, 5, sweeps // 2, lane), f32),
            pltpu.VMEM((chunks, 2, 3, sweeps // 2, lane), f32),
            pltpu.VMEM((chunks, 2, sweeps // 2, lane), f32),
            pltpu.VMEM((chunks, team + 1, sweeps, lane), f32),
            pltpu.VMEM((chunks, team, 2, sweeps, lane), f32),
            pltpu.VMEM((chunks, team, 2 * sweeps, lane), f32),
            pltpu.VMEM((height, width), f32),
            dma, dma, dma,
            dma((ncols - 1,)), dma((ncols - 1,)),
            dma((team - 1, ncols)), dma((team - 1,)),
            dma((team - 1, chunks)), dma((team - 1, chunks)),
            dma((4, ncols)), dma((4,)),
            dma((4, chunks)), dma((4, chunks)),
            dma((team - 1, chunks)), dma((team - 1, chunks)),
            dma((team - 1, chunks)), dma((team - 1, chunks)),
            pltpu.SemaphoreType.REGULAR, pltpu.SemaphoreType.REGULAR, pltpu.SemaphoreType.REGULAR,
        ],
        compiler_params=pltpu.CompilerParams(
            collective_id=0, has_side_effects=True, vmem_limit_bytes=32 * 1024 * 1024),
    )(*(pltpu.with_memory_space_constraint(a, pltpu.HBM)
        for a in (eigvecs, reflectors, starts.reshape(1, sweeps))))


def solution(mesh):
    in_specs = (P("rows", "cols"), P("cols", "rows"), P())
    out_specs = P("rows", "cols")
    body = functools.partial(per_device, mesh.shape["rows"], mesh.shape["cols"])
    return jax.shard_map(
        body, mesh=mesh, in_specs=in_specs, out_specs=out_specs, check_vma=False
    )
```

```python
import functools
import jax
import jax.numpy as jnp
from jax import lax
from jax.experimental import pallas as pl
from jax.experimental.pallas import tpu as pltpu
from jax.sharding import PartitionSpec as P

BAND = 64
LANES = 128
MESH = pl.DeviceIdType.MESH


def halves(a):
    high = a.astype(jnp.bfloat16)
    return high, (a - high.astype(jnp.float32)).astype(jnp.bfloat16)


def product(a, b, ca=1, cb=0):
    def one(left, right):
        return lax.dot_general(
            left, right, (((ca,), (cb,)), ((), ())), preferred_element_type=jnp.float32)
    return one(a[0], b[0]) + (one(a[0], b[1]) + one(a[1], b[0]))


def exact(a, b):
    left = jnp.concatenate(a, axis=1)
    right = jnp.concatenate(b, axis=1)
    both = lax.dot_general(
        left, jnp.concatenate([right, right], axis=0), (((1,), (0,)), ((), ())),
        preferred_element_type=jnp.float32)
    width = both.shape[1] // 2
    return both[:, :width] + both[:, width:]


def gram(a, b):
    return product(a, b, 1, 1) + lax.dot_general(
        a[1], b[1], (((1,), (1,)), ((), ())), preferred_element_type=jnp.float32)


def packed(a, sweeps):
    return a[:sweeps] + pltpu.roll(a[sweeps:], 2 * sweeps, 1)


def turn(a, by):
    return pltpu.roll(a, by % LANES, 1) if by % LANES else a


def unpacked(a, sweeps, by=0):
    inside = (lanes_of(a) - by) % LANES < 2 * sweeps
    return [jnp.where(inside, turn(a, by + side * 2 * sweeps), 0.0) for side in range(2)]


def lanes_of(a):
    return lax.broadcasted_iota(jnp.int32, a.shape, 1)


def sweep_pair(shape, sweeps):
    rows = lax.broadcasted_iota(jnp.int32, shape, 0) % sweeps
    cols = lax.broadcasted_iota(jnp.int32, shape, 1) % sweeps
    return rows, cols


def lower(full, sweeps):
    rows, cols = sweep_pair(full.shape, sweeps)
    return jnp.where(rows > cols, full, 0.0)


def on_diagonal(shape):
    return lax.broadcasted_iota(jnp.int32, shape, 0) == lax.broadcasted_iota(jnp.int32, shape, 1)


def seed(full, size):
    lanes = full.shape[1]
    rows = lax.broadcasted_iota(jnp.int32, full.shape, 0)
    cols = lax.broadcasted_iota(jnp.int32, full.shape, 1)
    own = jnp.where((rows ^ cols) < size, full, 0.0)
    below = [jnp.sum(jnp.where(rows - cols == m, own, 0.0), axis=0, keepdims=True)
             for m in range(size)]
    across = 1.0 / jnp.where(below[0] == 0.0, 1.0, below[0])

    def ahead(a, by):
        return pltpu.roll(a, lanes - by, 1) if by else a

    terms = [across]
    for k in range(1, size):
        total = sum(ahead(below[m], k - m) * terms[k - m] for m in range(1, k + 1))
        terms.append(-ahead(across, k) * total)
    done = jnp.where(rows == cols, across, 0.0)
    for k in range(1, size):
        done = jnp.where(rows - cols == k, terms[k], done)
    return done


def seed_pairs(full, sweeps, diag):
    eye = on_diagonal(full.shape)
    down = 1.0 / jnp.where(diag == 0.0, 1.0, diag)
    across = jnp.sum(jnp.where(eye, down, 0.0), axis=0, keepdims=True)
    rows, cols = sweep_pair(full.shape, sweeps)
    pair = ((rows ^ cols) == 1) & (rows > cols)
    return jnp.where(eye, down, 0.0) - down * jnp.where(pair, full, 0.0) * across


def inverse(full, sweeps, size, done, right=None):
    rows, cols = sweep_pair(full.shape, sweeps)
    apart = rows ^ cols
    while size < sweeps:
        reach = min(4 * size, sweeps)
        off = jnp.where((apart >= size) & (apart < reach) & (rows > cols), full, 0.0)
        inner = halves(done)
        step = halves(exact(inner, halves(off)))
        if reach == sweeps and right is not None:
            done = jnp.concatenate([done, exact(inner, right)], axis=1)
            inner = halves(done)
        first = done - exact(step, inner)
        if reach > 2 * size:
            twice = exact(step, step)
            first = first + exact(halves(twice), halves(first))
        done = first
        size = reach
    if right is None:
        return done
    return done[:, :full.shape[1]], done[:, full.shape[1]:]


def kernel(nrows, ncols, x_hbm, v_hbm, starts_hbm, out_ref, x_ref, v_all, starts_ref, lt_in, p_out,
           p_in, ltp_ref, ltp_in, follow, q_ref, near_in, far_in, z_all, z_in, y_in, ax_ref, x_sem, s_sem, v_local,
           v_send, v_recv, l_send, l_recv, p_send, p_recv, b_send, b_recv, q_send, q_recv, z_send, z_recv,
           y_send, y_recv, paired, entered, arrived):
    d, c = lax.axis_index("rows"), lax.axis_index("cols")
    own = v_hbm.shape[0]
    sweeps = v_all.shape[0]
    height, width = x_ref.shape
    depth = height // BAND
    chunks, team, _, lane = p_in.shape
    part = chunks * lane
    half = sweeps // 2
    group, member = d // team, d % team
    groups = nrows // team
    place = v_all.at[pl.ds(pl.multiple_of(c * own, own), own)]
    mine = pltpu.make_async_copy(v_hbm, place, v_local)
    mine.start()
    begins = pltpu.make_async_copy(starts_hbm, starts_ref, s_sem)
    begins.start()
    load = pltpu.make_async_copy(x_hbm, x_ref, x_sem)

    offsets = (-2, -1, 1, 2)
    far_first = sorted(enumerate(offsets), key=lambda item: -abs(item[1]))

    def there(offset):
        return group + offset >= 0 if offset < 0 else group + offset < groups

    def mate(step):
        return (member + step) % team

    last = ncols - 1
    base = group * team
    barrier = pltpu.get_barrier_semaphore()

    def greet(sem, slab, core):
        pl.semaphore_signal(sem, inc=1, device_id=(slab, core), device_id_type=MESH)

    @pl.when(c > 0)
    def _():
        greet(barrier, d, 0)

    @pl.when((member < team - 1) | (c < last))
    def _():
        greet(barrier, base + team - 1, last)
    for offset in offsets:
        @pl.when(there(offset))
        def _():
            greet(barrier, base + offset * team, last)
    z_all[:, 0] = jnp.zeros_like(z_all[:, 0])
    z_all[:, team] = jnp.zeros_like(z_all[:, 0])
    for i, offset in enumerate(offsets):
        @pl.when(jnp.logical_not(there(offset)))
        def _():
            ltp_in[i] = jnp.zeros_like(ltp_in[i])
            if abs(offset) == 1:
                near_in[:, i - 1] = jnp.zeros_like(near_in[:, 0])
            else:
                far_in[:, i // 3] = jnp.zeros_like(far_in[:, 0])
    load.start()

    @pl.when(c == 0)
    def _():
        pl.semaphore_wait(barrier, last)
        for core in range(1, ncols):
            greet(paired, d, core)

    @pl.when(c > 0)
    def _():
        pl.semaphore_wait(paired, 1)

    mine.wait()
    copies = []
    for step in range(1, ncols):
        copy = pltpu.make_async_remote_copy(
            src_ref=place, dst_ref=place, send_sem=v_send.at[step - 1], recv_sem=v_recv.at[step - 1],
            device_id=(d, (c + step) % ncols), device_id_type=MESH)
        copy.start()
        copies.append(copy)

    @pl.when((member == team - 1) & (c == last))
    def _():
        pl.semaphore_wait(barrier, ncols * team - 1)
        for slab in range(team):
            for core in range(ncols):
                if slab < team - 1 or core < last:
                    greet(entered, base + slab, core)

    begins.wait()
    across = jnp.broadcast_to(starts_ref[...], (sweeps, sweeps))
    begin = jnp.sum(jnp.where(on_diagonal(across.shape), across, 0), axis=1, keepdims=True)
    row = lax.broadcasted_iota(jnp.int32, v_all.shape, 1)
    window = (row - begin + BAND) // BAND
    outside = ((window == 0) & (d == 0)) | ((window == depth) & (d == nrows - 1) & (begin > 0))
    for copy in copies:
        copy.wait_recv()

    v = v_all[...]
    v = jnp.where(outside, 0.0, v)
    parts = [jnp.where(window == k, v, 0.0) for k in range(depth + 1)]
    u_s = jnp.concatenate([parts[0], parts[depth]], axis=0)
    u_i = jnp.concatenate(parts[1:depth], axis=0)
    inside = u_i.shape[0]
    edge = 2 * sweeps
    half_s = 0.5 * jnp.sum(u_s * u_s, axis=1, keepdims=True)
    half_i = 0.5 * jnp.sum(u_i * u_i, axis=1, keepdims=True)
    half_i = jnp.concatenate([half_i, jnp.zeros((LANES - inside, 1), jnp.float32)], axis=0)
    pad = jnp.zeros((LANES - edge, height), jnp.float32)
    us_h, ui_h = halves(u_s), halves(u_i)
    all_h = halves(jnp.concatenate(
        [u_i, jnp.zeros((LANES - inside, height), jnp.float32), u_s, pad], axis=0))
    g = gram(tuple(a[:LANES + edge] for a in all_h), all_h)
    g_ii, n_is = g[:LANES, :LANES], lower(g[:LANES, LANES:], sweeps)
    n_si, g_ss = lower(g[LANES:, :LANES], sweeps), g[LANES:, LANES:]
    l_ii = jnp.where(on_diagonal(g_ii.shape), half_i, lower(g_ii, sweeps))
    n_ss = jnp.where(on_diagonal(g_ss.shape), half_s, lower(g_ss, sweeps))
    t, f = inverse(l_ii, sweeps, 2, seed_pairs(l_ii, sweeps, half_i), halves(n_is))
    nsi_h = halves(n_si)
    lt_in[member] = packed(n_ss - exact(nsi_h, halves(f)), sweeps)
    t_h = halves(t)
    k_h = tuple(a[:, :inside] for a in halves(exact(nsi_h, t_h)))
    t_h = tuple(a[:inside, :inside] for a in t_h)

    def to_mate(step, src, dst, send, recv):
        return pltpu.make_async_remote_copy(
            src_ref=src, dst_ref=dst, send_sem=send, recv_sem=recv,
            device_id=(base + mate(step), c), device_id_type=MESH)

    def lt_copy(step, core):
        return pltpu.make_async_remote_copy(
            src_ref=lt_in.at[member], dst_ref=lt_in.at[member], send_sem=l_send.at[step - 1, core],
            recv_sem=l_recv.at[step - 1], device_id=(base + mate(step), core), device_id_type=MESH)

    def p_copy(step, ch):
        return to_mate(step, p_out.at[ch, mate(step)], p_in.at[ch, member],
                       p_send.at[step - 1, ch], p_recv.at[step - 1, ch])

    def z_copy(step, ch):
        return to_mate(step, z_all.at[ch, pl.ds(mate(step), 2)], z_in.at[ch, member],
                       z_send.at[step - 1, ch], z_recv.at[step - 1, ch])

    read = -(-(edge - depth * (team - 1)) // 8) * 8

    def reads(j):
        return depth * j // 8 * 8

    def y_copy(step, ch):
        rows = pl.ds(pl.multiple_of(reads(mate(step)), 8), read)
        return to_mate(step, y_in.at[ch, member, rows], y_in.at[ch, member, rows],
                       y_send.at[step - 1, ch], y_recv.at[step - 1, ch])

    def b_copy(i, slot, core):
        return pltpu.make_async_remote_copy(
            src_ref=ltp_ref.at[i // 2], dst_ref=ltp_in.at[slot], send_sem=b_send.at[i, core],
            recv_sem=b_recv.at[slot], device_id=(d + offsets[i] * team, core), device_id_type=MESH)

    def q_copy(i, slot, ch):
        if offsets[i] == -2:
            src, dst = q_ref.at[ch, 0], far_in.at[ch, 1]
        elif offsets[i] == -1:
            src, dst = q_ref.at[ch, pl.ds(0, 3)], near_in.at[ch, 1]
        elif offsets[i] == 1:
            src, dst = q_ref.at[ch, pl.ds(2, 3)], near_in.at[ch, 0]
        else:
            src, dst = q_ref.at[ch, 2], far_in.at[ch, 0]
        return pltpu.make_async_remote_copy(
            src_ref=src, dst_ref=dst, send_sem=q_send.at[i, ch], recv_sem=q_recv.at[slot, ch],
            device_id=(d + offsets[i] * team, c), device_id_type=MESH)

    @pl.when((member < team - 1) | (c < last))
    def _():
        pl.semaphore_wait(entered, 1)

    @pl.when(c == last)
    def _():
        for core in range(ncols):
            for step in range(1, team):
                lt_copy(step, core).start()

    load.wait()
    span = team * lane
    slices = [slice(ch * span, (ch + 1) * span) for ch in range(chunks)]
    wi_h = []
    for ch in range(chunks):
        x_h = halves(x_ref[:, slices[ch]])
        wi_h.append(halves(product(ui_h, x_h)))
        p = product(us_h, x_h) - product(k_h, wi_h[ch])
        for j in range(team):
            p_out[ch, j] = p[:, j * lane:(j + 1) * lane]
        for step in range(1, team):
            p_copy(step, ch).start()
        p_in[ch, member] = p_out[ch, member]

    peers = sum(there(offset).astype(jnp.int32) for offset in offsets)

    @pl.when((member == 0) & (c == last))
    def _():
        pl.semaphore_wait(barrier, peers * ncols * team)
        for slab in range(team):
            for core in range(ncols):
                if slab > 0 or core < last:
                    greet(arrived, base + slab, core)

    u_t = u_i.T
    ut_h = halves(u_t)
    for ch, cols in enumerate(slices):
        inner = product(t_h, wi_h[ch])
        ax_ref[:, cols] = x_ref[:, cols] - product(ut_h, halves(inner))
    cm_h = halves(u_s.T - product(ut_h, halves(f[:inside, :edge])))

    for step in range(1, team):
        lt_copy(step, 0).wait_recv()
    zero = jnp.zeros((sweeps, LANES), jnp.float32)
    blocks = [zero] * (team + 1)
    for j in range(team):
        for side, rows in enumerate(unpacked(lt_in[j], sweeps, j * sweeps)):
            blocks[j + side] = blocks[j + side] + rows
    first = lanes_of(blocks[0]) < sweeps
    keep = [jnp.where(first, 0.0, block) for block in blocks]
    ends = [jnp.where(first, block, 0.0) for block in blocks]
    m_ii = jnp.concatenate([zero] + keep[1:team], axis=0)
    m_si = jnp.concatenate([keep[0], keep[team]], axis=0)
    left = [zero] * team
    left[1] = left[1] + ends[1]
    left[team - 1] = left[team - 1] + pltpu.roll(ends[team - 1], sweeps, 1)
    m_is = jnp.concatenate(left, axis=0)
    m_ss = jnp.concatenate([ends[0], pltpu.roll(ends[team], sweeps, 1)], axis=0)
    tt, ff = inverse(m_ii, sweeps, depth, seed(m_ii, depth), halves(m_is))
    msi_h = halves(m_si)
    ltp = m_ss - exact(msi_h, halves(ff))
    at_l, at_r = ltp[:sweeps], ltp[sweeps:]
    early = lax.broadcasted_iota(jnp.int32, zero.shape, 0) < half
    beside = (lanes_of(zero) >= sweeps) & (lanes_of(zero) < sweeps + half)
    to_left = jnp.where(first, at_l, jnp.where(beside, jnp.where(early, at_r, at_l), 0.0))
    to_right = jnp.where(first, turn(at_r, -sweeps), jnp.where(
        beside, turn(jnp.where(early, at_l, at_r), sweeps), 0.0))
    for side, rows in enumerate((to_left, to_right)):
        ltp_ref[side] = rows[:half] + turn(rows[half:], edge)
    @pl.when((member > 0) | (c < last))
    def _():
        pl.semaphore_wait(arrived, 1)

    for i, offset in far_first:
        @pl.when(there(offset) & (c == last))
        def _():
            for core in range(ncols):
                b_copy(i, 3 - i, core).start()
    tt_h = halves(tt)
    kk_h = halves(exact(msi_h, tt_h))
    for ch in range(chunks):
        for step in range(1, team):
            p_copy(step, ch).wait_recv()
        rows = [jnp.zeros((sweeps, lane), jnp.float32)]
        for j in range(1, team):
            rows.append(p_in[ch, j - 1, sweeps:] + p_in[ch, j, :sweeps])
        q_i = halves(jnp.concatenate(rows, axis=0))
        q_s = jnp.concatenate([p_in[ch, 0, :sweeps], p_in[ch, team - 1, sweeps:]], axis=0)
        q = q_s - product(kk_h, q_i)
        for j in range(4):
            q_ref[ch, j] = q[j * half:(j + 1) * half]
        q_ref[ch, 4] = q[:half]
        for i, offset in far_first:
            @pl.when(there(offset))
            def _():
                q_copy(i, 3 - i, ch).start()
        z_i = product(tt_h, q_i)
        for j in range(1, team):
            z_all[ch, j] = z_i[j * sweeps:(j + 1) * sweeps]
        for step in range(1, team):
            z_copy(step, ch).start()
    new = lanes_of(m_ii)
    new = jnp.where(new < sweeps, sweeps - 8 - new + 2 * (new % 8), new)
    order = (lax.broadcasted_iota(jnp.int32, new.shape, 0) == new).astype(jnp.bfloat16)
    ff = sum(lax.dot_general(a, order, (((1,), (0,)), ((), ())), preferred_element_type=jnp.float32)
             for a in halves(ff))
    follow[0] = order[:sweeps].astype(jnp.float32)
    for j in range(1, team):
        follow[j] = -ff[j * sweeps:(j + 1) * sweeps]
    follow[team] = order[sweeps:edge].astype(jnp.float32)
    mine_h = halves(follow[pl.ds(member, 2)].reshape(edge, LANES))
    cf_h = halves(product(cm_h, mine_h)[:, :edge])
    cf3 = jnp.concatenate([cf_h[0], cf_h[1], cf_h[0]], axis=1)

    for i, offset in enumerate(offsets):
        @pl.when(there(offset))
        def _():
            b_copy(i, i, 0).wait_recv()
    def at(rows, low, high):
        return jnp.where((lanes_of(rows) >= low) & (lanes_of(rows) < high), rows, 0.0)

    far_l, near_l, near_r, far_r = (ltp_in[i] for i in range(4))
    up, down = turn(near_l, sweeps), turn(near_l, -sweeps)
    late = jnp.zeros((half, LANES), jnp.float32)
    big = jnp.concatenate([
        at(far_l + down, 0, half),
        late,
        at(up, sweeps, 2 * sweeps),
        at(down, sweeps, 2 * sweeps) + at(up, 0, half),
        at(turn(near_r, 2 * sweeps), 2 * sweeps, 3 * sweeps),
        at(near_r, 2 * sweeps, 3 * sweeps + half),
        at(turn(near_r, 2 * sweeps) + turn(far_r, 3 * sweeps), 3 * sweeps, 3 * sweeps + half),
        late,
    ], axis=0)
    here = turn(ltp, sweeps)
    big = big + jnp.concatenate([zero, here, zero], axis=0)
    def own_rows(a):
        blocks = [a[b:b + 8] for b in range(2 * sweeps - 8, sweeps - 1, -8)]
        return jnp.concatenate(blocks + [a[2 * sweeps:3 * sweeps]], axis=0)

    apart = [axis & (sweeps - 1) for axis in (
        lax.broadcasted_iota(jnp.int32, big.shape, 0), lax.broadcasted_iota(jnp.int32, big.shape, 1))]
    off = jnp.where((apart[0] >= half) & (apart[1] < half), big, 0.0)
    done = seed(big, half)
    near = own_rows(done)
    step = exact(halves(near), halves(off))
    s_h = halves(near - exact(halves(step), halves(done)))

    none = jnp.zeros((half, lane), jnp.float32)
    for ch in range(chunks):
        for i, offset in enumerate(offsets):
            @pl.when(there(offset))
            def _():
                q_copy(i, i, ch).wait_recv()
        rhs = jnp.concatenate([
            far_in[ch, 0] + near_in[ch, 0, 2],
            none,
            near_in[ch, 0, 0] + q_ref[ch, 0],
            near_in[ch, 0, 1] + q_ref[ch, 1],
            q_ref[ch, 2] + near_in[ch, 1, 0],
            q_ref[ch, 3] + near_in[ch, 1, 1],
            near_in[ch, 1, 2] + far_in[ch, 1],
            none,
        ], axis=0)
        y_in[ch, member] = product(s_h, halves(rhs))
        for step in range(1, team):
            y_copy(step, ch).start()

    cm3 = jnp.concatenate([cm_h[0], cm_h[1], cm_h[0]], axis=1)

    def apply(left, y):
        y_h = halves(y)
        y3 = jnp.concatenate([y_h[0], y_h[0], y_h[1]], axis=0)
        return lax.dot_general(left, y3, (((1,), (0,)), ((), ())), preferred_element_type=jnp.float32)

    for ch in range(chunks):
        z_in[ch, member] = z_all[ch, pl.ds(member, 2)]
    for ch, cols in enumerate(slices):
        for step in range(1, team):
            z_copy(step, ch).wait_recv()
        z = jnp.concatenate([z_in[ch, j].reshape(edge, lane) for j in range(team)], axis=1)
        ax_ref[:, cols] = ax_ref[:, cols] - apply(cm3, z)

    row = lax.broadcasted_iota(jnp.int32, (edge, lane), 0)
    sent = (row >= reads(member)) & (row < reads(member) + read)

    for ch in range(chunks - 1):
        for step in range(1, team):
            y_copy(step, ch).wait_recv()
        cols = slices[ch]
        y = jnp.concatenate([jnp.where(sent, y_in[ch, j], 0.0) for j in range(team)], axis=1)
        out_ref[:, cols] = ax_ref[:, cols] - apply(cf3, y)

    def last_step(j):
        cols = pl.ds(pl.multiple_of(((chunks - 1) * team + j) * lane, lane), lane)
        out_ref[:, cols] = ax_ref[:, cols] - apply(cf3, jnp.where(sent, y_in[chunks - 1, j], 0.0))

    last_step(member)
    for step in range(1, team):
        y_copy(step, chunks - 1).wait_recv()
        last_step(mate(team - step))

    for copy in copies:
        copy.wait_send()
    for step in range(1, team):
        for ch in range(chunks):
            p_copy(step, ch).wait_send()
            z_copy(step, ch).wait_send()
            y_copy(step, ch).wait_send()
    for i, offset in enumerate(offsets):
        @pl.when(there(offset))
        def _():
            for ch in range(chunks):
                q_copy(i, 3 - i, ch).wait_send()

    @pl.when(c == last)
    def _():
        for core in range(ncols):
            for step in range(1, team):
                lt_copy(step, core).wait_send()
            for i, offset in enumerate(offsets):
                @pl.when(there(offset))
                def _():
                    b_copy(i, 3 - i, core).wait_send()


def per_device(nrows, ncols, eigvecs, reflectors, starts):
    height, width = eigvecs.shape
    sweeps = starts.shape[0]
    team = sweeps // (2 * (height // BAND))
    part = width // team
    lane = LANES
    chunks = part // lane
    assert team * sweeps == LANES and nrows % team == 0
    f32 = jnp.float32
    hbm = pl.BlockSpec(memory_space=pltpu.HBM)
    dma = pltpu.SemaphoreType.DMA
    return pl.pallas_call(
        functools.partial(kernel, nrows, ncols),
        out_shape=jax.ShapeDtypeStruct((height, width), f32),
        in_specs=[hbm, hbm, hbm],
        out_specs=pl.BlockSpec(memory_space=pltpu.VMEM),
        scratch_shapes=[
            pltpu.VMEM((height, width), f32),
            pltpu.VMEM((sweeps, height), f32),
            pltpu.VMEM((1, sweeps), jnp.int32),
            pltpu.VMEM((team, sweeps, LANES), f32),
            pltpu.VMEM((chunks, team, 2 * sweeps, lane), f32),
            pltpu.VMEM((chunks, team, 2 * sweeps, lane), f32),
            pltpu.VMEM((2, sweeps // 2, LANES), f32),
            pltpu.VMEM((4, sweeps // 2, LANES), f32),
            pltpu.VMEM((team + 1, sweeps, LANES), f32),
            pltpu.VMEM((chunks, 5, sweeps // 2, lane), f32),
            pltpu.VMEM((chunks, 2, 3, sweeps // 2, lane), f32),
            pltpu.VMEM((chunks, 2, sweeps // 2, lane), f32),
            pltpu.VMEM((chunks, team + 1, sweeps, lane), f32),
            pltpu.VMEM((chunks, team, 2, sweeps, lane), f32),
            pltpu.VMEM((chunks, team, 2 * sweeps, lane), f32),
            pltpu.VMEM((height, width), f32),
            dma, dma, dma,
            dma((ncols - 1,)), dma((ncols - 1,)),
            dma((team - 1, ncols)), dma((team - 1,)),
            dma((team - 1, chunks)), dma((team - 1, chunks)),
            dma((4, ncols)), dma((4,)),
            dma((4, chunks)), dma((4, chunks)),
            dma((team - 1, chunks)), dma((team - 1, chunks)),
            dma((team - 1, chunks)), dma((team - 1, chunks)),
            pltpu.SemaphoreType.REGULAR, pltpu.SemaphoreType.REGULAR, pltpu.SemaphoreType.REGULAR,
        ],
        compiler_params=pltpu.CompilerParams(
            collective_id=0, has_side_effects=True, vmem_limit_bytes=32 * 1024 * 1024),
    )(*(pltpu.with_memory_space_constraint(a, pltpu.HBM)
        for a in (eigvecs, reflectors, starts.reshape(1, sweeps))))


def solution(mesh):
    in_specs = (P("rows", "cols"), P("cols", "rows"), P())
    out_specs = P("rows", "cols")
    body = functools.partial(per_device, mesh.shape["rows"], mesh.shape["cols"])
    return jax.shard_map(
        body, mesh=mesh, in_specs=in_specs, out_specs=out_specs, check_vma=False
    )
```

```python
import functools
import jax
import jax.numpy as jnp
from jax import lax
from jax.experimental import pallas as pl
from jax.experimental.pallas import tpu as pltpu
from jax.sharding import PartitionSpec as P

BAND = 64
LANES = 128
MESH = pl.DeviceIdType.MESH


def halves(a):
    high = a.astype(jnp.bfloat16)
    return high, (a - high.astype(jnp.float32)).astype(jnp.bfloat16)


def product(a, b, ca=1, cb=0):
    def one(left, right):
        return lax.dot_general(
            left, right, (((ca,), (cb,)), ((), ())), preferred_element_type=jnp.float32)
    return one(a[0], b[0]) + (one(a[0], b[1]) + one(a[1], b[0]))


def exact(a, b):
    left = jnp.concatenate(a, axis=1)
    right = jnp.concatenate(b, axis=1)
    both = lax.dot_general(
        left, jnp.concatenate([right, right], axis=0), (((1,), (0,)), ((), ())),
        preferred_element_type=jnp.float32)
    width = both.shape[1] // 2
    return both[:, :width] + both[:, width:]


def gram(a, b):
    return product(a, b, 1, 1) + lax.dot_general(
        a[1], b[1], (((1,), (1,)), ((), ())), preferred_element_type=jnp.float32)


def packed(a, sweeps):
    return a[:sweeps] + pltpu.roll(a[sweeps:], 2 * sweeps, 1)


def turn(a, by):
    return pltpu.roll(a, by % LANES, 1) if by % LANES else a


def unpacked(a, sweeps, by=0):
    inside = (lanes_of(a) - by) % LANES < 2 * sweeps
    return [jnp.where(inside, turn(a, by + side * 2 * sweeps), 0.0) for side in range(2)]


def lanes_of(a):
    return lax.broadcasted_iota(jnp.int32, a.shape, 1)


def sweep_pair(shape, sweeps):
    rows = lax.broadcasted_iota(jnp.int32, shape, 0) % sweeps
    cols = lax.broadcasted_iota(jnp.int32, shape, 1) % sweeps
    return rows, cols


def lower(full, sweeps):
    rows, cols = sweep_pair(full.shape, sweeps)
    return jnp.where(rows > cols, full, 0.0)


def on_diagonal(shape):
    return lax.broadcasted_iota(jnp.int32, shape, 0) == lax.broadcasted_iota(jnp.int32, shape, 1)


def seed(full, size):
    lanes = full.shape[1]
    rows = lax.broadcasted_iota(jnp.int32, full.shape, 0)
    cols = lax.broadcasted_iota(jnp.int32, full.shape, 1)
    own = jnp.where((rows ^ cols) < size, full, 0.0)
    below = [jnp.sum(jnp.where(rows - cols == m, own, 0.0), axis=0, keepdims=True)
             for m in range(size)]
    across = 1.0 / jnp.where(below[0] == 0.0, 1.0, below[0])

    def ahead(a, by):
        return pltpu.roll(a, lanes - by, 1) if by else a

    terms = [across]
    for k in range(1, size):
        total = sum(ahead(below[m], k - m) * terms[k - m] for m in range(1, k + 1))
        terms.append(-ahead(across, k) * total)
    done = jnp.where(rows == cols, across, 0.0)
    for k in range(1, size):
        done = jnp.where(rows - cols == k, terms[k], done)
    return done


def seed_pairs(full, sweeps, diag):
    eye = on_diagonal(full.shape)
    down = 1.0 / jnp.where(diag == 0.0, 1.0, diag)
    across = jnp.sum(jnp.where(eye, down, 0.0), axis=0, keepdims=True)
    rows, cols = sweep_pair(full.shape, sweeps)
    pair = ((rows ^ cols) == 1) & (rows > cols)
    return jnp.where(eye, down, 0.0) - down * jnp.where(pair, full, 0.0) * across


def inverse(full, sweeps, size, done, right=None):
    rows, cols = sweep_pair(full.shape, sweeps)
    apart = rows ^ cols
    while size < sweeps:
        reach = min(4 * size, sweeps)
        off = jnp.where((apart >= size) & (apart < reach) & (rows > cols), full, 0.0)
        inner = halves(done)
        step = halves(exact(inner, halves(off)))
        if reach == sweeps and right is not None:
            done = jnp.concatenate([done, exact(inner, right)], axis=1)
            inner = halves(done)
        first = done - exact(step, inner)
        if reach > 2 * size:
            twice = exact(step, step)
            first = first + exact(halves(twice), halves(first))
        done = first
        size = reach
    if right is None:
        return done
    return done[:, :full.shape[1]], done[:, full.shape[1]:]


def kernel(nrows, ncols, x_hbm, v_hbm, starts_hbm, out_ref, x_ref, v_all, starts_ref, lt_in, p_out,
           p_in, ltp_ref, ltp_in, follow, q_ref, near_in, far_in, z_all, z_in, y_in, ax_ref, x_sem, s_sem, v_local,
           v_send, v_recv, l_send, l_recv, p_send, p_recv, b_send, b_recv, q_send, q_recv, z_send, z_recv,
           y_send, y_recv, paired, entered, arrived):
    d, c = lax.axis_index("rows"), lax.axis_index("cols")
    own = v_hbm.shape[0]
    sweeps = v_all.shape[0]
    height, width = x_ref.shape
    depth = height // BAND
    chunks, team, _, lane = p_in.shape
    part = chunks * lane
    half = sweeps // 2
    group, member = d // team, d % team
    groups = nrows // team
    place = v_all.at[pl.ds(pl.multiple_of(c * own, own), own)]
    mine = pltpu.make_async_copy(v_hbm, place, v_local)
    mine.start()
    begins = pltpu.make_async_copy(starts_hbm, starts_ref, s_sem)
    begins.start()
    load = pltpu.make_async_copy(x_hbm, x_ref, x_sem)

    offsets = (-2, -1, 1, 2)
    far_mates = sorted(range(1, team), key=lambda step: step % 2 == 0)
    far_first = sorted(enumerate(offsets), key=lambda item: -abs(item[1]))

    def there(offset):
        return group + offset >= 0 if offset < 0 else group + offset < groups

    def mate(step):
        return (member + step) % team

    last = ncols - 1
    base = group * team
    barrier = pltpu.get_barrier_semaphore()

    def greet(sem, slab, core):
        pl.semaphore_signal(sem, inc=1, device_id=(slab, core), device_id_type=MESH)

    @pl.when(c > 0)
    def _():
        greet(barrier, d, 0)

    @pl.when((member < team - 1) | (c < last))
    def _():
        greet(barrier, base + team - 1, last)
    for offset in offsets:
        @pl.when(there(offset))
        def _():
            greet(barrier, base + offset * team, last)
    z_all[:, 0] = jnp.zeros_like(z_all[:, 0])
    z_all[:, team] = jnp.zeros_like(z_all[:, 0])
    for i, offset in enumerate(offsets):
        @pl.when(jnp.logical_not(there(offset)))
        def _():
            ltp_in[i] = jnp.zeros_like(ltp_in[i])
            if abs(offset) == 1:
                near_in[:, i - 1] = jnp.zeros_like(near_in[:, 0])
            else:
                far_in[:, i // 3] = jnp.zeros_like(far_in[:, 0])
    load.start()

    @pl.when(c == 0)
    def _():
        pl.semaphore_wait(barrier, last)
        for core in range(1, ncols):
            greet(paired, d, core)

    @pl.when(c > 0)
    def _():
        pl.semaphore_wait(paired, 1)

    mine.wait()
    copies = []
    for step in range(1, ncols):
        copy = pltpu.make_async_remote_copy(
            src_ref=place, dst_ref=place, send_sem=v_send.at[step - 1], recv_sem=v_recv.at[step - 1],
            device_id=(d, (c + step) % ncols), device_id_type=MESH)
        copy.start()
        copies.append(copy)

    @pl.when((member == team - 1) & (c == last))
    def _():
        pl.semaphore_wait(barrier, ncols * team - 1)
        for slab in range(team):
            for core in range(ncols):
                if slab < team - 1 or core < last:
                    greet(entered, base + slab, core)

    begins.wait()
    across = jnp.broadcast_to(starts_ref[...], (sweeps, sweeps))
    begin = jnp.sum(jnp.where(on_diagonal(across.shape), across, 0), axis=1, keepdims=True)
    row = lax.broadcasted_iota(jnp.int32, v_all.shape, 1)
    window = (row - begin + BAND) // BAND
    outside = ((window == 0) & (d == 0)) | ((window == depth) & (d == nrows - 1) & (begin > 0))
    for copy in copies:
        copy.wait_recv()

    v = v_all[...]
    v = jnp.where(outside, 0.0, v)
    parts = [jnp.where(window == k, v, 0.0) for k in range(depth + 1)]
    u_s = jnp.concatenate([parts[0], parts[depth]], axis=0)
    u_i = jnp.concatenate(parts[1:depth], axis=0)
    inside = u_i.shape[0]
    edge = 2 * sweeps
    half_s = 0.5 * jnp.sum(u_s * u_s, axis=1, keepdims=True)
    half_i = 0.5 * jnp.sum(u_i * u_i, axis=1, keepdims=True)
    half_i = jnp.concatenate([half_i, jnp.zeros((LANES - inside, 1), jnp.float32)], axis=0)
    pad = jnp.zeros((LANES - edge, height), jnp.float32)
    us_h, ui_h = halves(u_s), halves(u_i)
    all_h = halves(jnp.concatenate(
        [u_i, jnp.zeros((LANES - inside, height), jnp.float32), u_s, pad], axis=0))
    g = gram(tuple(a[:LANES + edge] for a in all_h), all_h)
    g_ii, n_is = g[:LANES, :LANES], lower(g[:LANES, LANES:], sweeps)
    n_si, g_ss = lower(g[LANES:, :LANES], sweeps), g[LANES:, LANES:]
    l_ii = jnp.where(on_diagonal(g_ii.shape), half_i, lower(g_ii, sweeps))
    n_ss = jnp.where(on_diagonal(g_ss.shape), half_s, lower(g_ss, sweeps))
    t, f = inverse(l_ii, sweeps, 2, seed_pairs(l_ii, sweeps, half_i), halves(n_is))
    nsi_h = halves(n_si)
    lt_in[member] = packed(n_ss - exact(nsi_h, halves(f)), sweeps)
    t_h = halves(t)
    k_h = tuple(a[:, :inside] for a in halves(exact(nsi_h, t_h)))
    t_h = tuple(a[:inside, :inside] for a in t_h)

    def to_mate(step, src, dst, send, recv):
        return pltpu.make_async_remote_copy(
            src_ref=src, dst_ref=dst, send_sem=send, recv_sem=recv,
            device_id=(base + mate(step), c), device_id_type=MESH)

    def lt_copy(step, core):
        return pltpu.make_async_remote_copy(
            src_ref=lt_in.at[member], dst_ref=lt_in.at[member], send_sem=l_send.at[step - 1, core],
            recv_sem=l_recv.at[step - 1], device_id=(base + mate(step), core), device_id_type=MESH)

    def p_copy(step, ch):
        return to_mate(step, p_out.at[ch, mate(step)], p_in.at[ch, member],
                       p_send.at[step - 1, ch], p_recv.at[step - 1, ch])

    def z_copy(step, ch):
        return to_mate(step, z_all.at[ch, pl.ds(mate(step), 2)], z_in.at[ch, member],
                       z_send.at[step - 1, ch], z_recv.at[step - 1, ch])

    read = -(-(edge - depth * (team - 1)) // 8) * 8

    def reads(j):
        return depth * j // 8 * 8

    def y_copy(step, ch):
        rows = pl.ds(pl.multiple_of(reads(mate(step)), 8), read)
        return to_mate(step, y_in.at[ch, member, rows], y_in.at[ch, member, rows],
                       y_send.at[step - 1, ch], y_recv.at[step - 1, ch])

    def b_copy(i, slot, core):
        return pltpu.make_async_remote_copy(
            src_ref=ltp_ref.at[i // 2], dst_ref=ltp_in.at[slot], send_sem=b_send.at[i, core],
            recv_sem=b_recv.at[slot], device_id=(d + offsets[i] * team, core), device_id_type=MESH)

    def q_copy(i, slot, ch):
        if offsets[i] == -2:
            src, dst = q_ref.at[ch, 0], far_in.at[ch, 1]
        elif offsets[i] == -1:
            src, dst = q_ref.at[ch, pl.ds(0, 3)], near_in.at[ch, 1]
        elif offsets[i] == 1:
            src, dst = q_ref.at[ch, pl.ds(2, 3)], near_in.at[ch, 0]
        else:
            src, dst = q_ref.at[ch, 2], far_in.at[ch, 0]
        return pltpu.make_async_remote_copy(
            src_ref=src, dst_ref=dst, send_sem=q_send.at[i, ch], recv_sem=q_recv.at[slot, ch],
            device_id=(d + offsets[i] * team, c), device_id_type=MESH)

    @pl.when((member < team - 1) | (c < last))
    def _():
        pl.semaphore_wait(entered, 1)

    @pl.when(c == last)
    def _():
        for core in range(ncols):
            for step in range(1, team):
                lt_copy(step, core).start()

    load.wait()
    span = team * lane
    slices = [slice(ch * span, (ch + 1) * span) for ch in range(chunks)]
    wi_h = []
    for ch in range(chunks):
        x_h = halves(x_ref[:, slices[ch]])
        wi_h.append(halves(product(ui_h, x_h)))
        p = product(us_h, x_h) - product(k_h, wi_h[ch])
        for j in range(team):
            p_out[ch, j] = p[:, j * lane:(j + 1) * lane]
        for step in far_mates:
            p_copy(step, ch).start()
        p_in[ch, member] = p_out[ch, member]

    peers = sum(there(offset).astype(jnp.int32) for offset in offsets)

    @pl.when((member == 0) & (c == last))
    def _():
        pl.semaphore_wait(barrier, peers * ncols * team)
        for slab in range(team):
            for core in range(ncols):
                if slab > 0 or core < last:
                    greet(arrived, base + slab, core)

    u_t = u_i.T
    ut_h = halves(u_t)
    for ch, cols in enumerate(slices):
        inner = product(t_h, wi_h[ch])
        ax_ref[:, cols] = x_ref[:, cols] - product(ut_h, halves(inner))
    cm_h = halves(u_s.T - product(ut_h, halves(f[:inside, :edge])))

    for step in range(1, team):
        lt_copy(step, 0).wait_recv()
    zero = jnp.zeros((sweeps, LANES), jnp.float32)
    blocks = [zero] * (team + 1)
    for j in range(team):
        for side, rows in enumerate(unpacked(lt_in[j], sweeps, j * sweeps)):
            blocks[j + side] = blocks[j + side] + rows
    first = lanes_of(blocks[0]) < sweeps
    keep = [jnp.where(first, 0.0, block) for block in blocks]
    ends = [jnp.where(first, block, 0.0) for block in blocks]
    m_ii = jnp.concatenate([zero] + keep[1:team], axis=0)
    m_si = jnp.concatenate([keep[0], keep[team]], axis=0)
    left = [zero] * team
    left[1] = left[1] + ends[1]
    left[team - 1] = left[team - 1] + pltpu.roll(ends[team - 1], sweeps, 1)
    m_is = jnp.concatenate(left, axis=0)
    m_ss = jnp.concatenate([ends[0], pltpu.roll(ends[team], sweeps, 1)], axis=0)
    tt, ff = inverse(m_ii, sweeps, depth, seed(m_ii, depth), halves(m_is))
    msi_h = halves(m_si)
    ltp = m_ss - exact(msi_h, halves(ff))
    at_l, at_r = ltp[:sweeps], ltp[sweeps:]
    early = lax.broadcasted_iota(jnp.int32, zero.shape, 0) < half
    beside = (lanes_of(zero) >= sweeps) & (lanes_of(zero) < sweeps + half)
    to_left = jnp.where(first, at_l, jnp.where(beside, jnp.where(early, at_r, at_l), 0.0))
    to_right = jnp.where(first, turn(at_r, -sweeps), jnp.where(
        beside, turn(jnp.where(early, at_l, at_r), sweeps), 0.0))
    for side, rows in enumerate((to_left, to_right)):
        ltp_ref[side] = rows[:half] + turn(rows[half:], edge)
    @pl.when((member > 0) | (c < last))
    def _():
        pl.semaphore_wait(arrived, 1)

    for i, offset in far_first:
        @pl.when(there(offset) & (c == last))
        def _():
            for core in range(ncols):
                b_copy(i, 3 - i, core).start()
    tt_h = halves(tt)
    kk_h = halves(exact(msi_h, tt_h))
    for ch in range(chunks):
        for step in range(1, team):
            p_copy(step, ch).wait_recv()
        rows = [jnp.zeros((sweeps, lane), jnp.float32)]
        for j in range(1, team):
            rows.append(p_in[ch, j - 1, sweeps:] + p_in[ch, j, :sweeps])
        q_i = halves(jnp.concatenate(rows, axis=0))
        q_s = jnp.concatenate([p_in[ch, 0, :sweeps], p_in[ch, team - 1, sweeps:]], axis=0)
        q = q_s - product(kk_h, q_i)
        for j in range(4):
            q_ref[ch, j] = q[j * half:(j + 1) * half]
        q_ref[ch, 4] = q[:half]
        for i, offset in far_first:
            @pl.when(there(offset))
            def _():
                q_copy(i, 3 - i, ch).start()
        z_i = product(tt_h, q_i)
        for j in range(1, team):
            z_all[ch, j] = z_i[j * sweeps:(j + 1) * sweeps]
        for step in range(1, team):
            z_copy(step, ch).start()
    new = lanes_of(m_ii)
    new = jnp.where(new < sweeps, sweeps - 8 - new + 2 * (new % 8), new)
    order = (lax.broadcasted_iota(jnp.int32, new.shape, 0) == new).astype(jnp.bfloat16)
    ff = sum(lax.dot_general(a, order, (((1,), (0,)), ((), ())), preferred_element_type=jnp.float32)
             for a in halves(ff))
    follow[0] = order[:sweeps].astype(jnp.float32)
    for j in range(1, team):
        follow[j] = -ff[j * sweeps:(j + 1) * sweeps]
    follow[team] = order[sweeps:edge].astype(jnp.float32)
    mine_h = halves(follow[pl.ds(member, 2)].reshape(edge, LANES))
    cf_h = halves(product(cm_h, mine_h)[:, :edge])
    cf3 = jnp.concatenate([cf_h[0], cf_h[1], cf_h[0]], axis=1)

    for i, offset in enumerate(offsets):
        @pl.when(there(offset))
        def _():
            b_copy(i, i, 0).wait_recv()
    def at(rows, low, high):
        return jnp.where((lanes_of(rows) >= low) & (lanes_of(rows) < high), rows, 0.0)

    far_l, near_l, near_r, far_r = (ltp_in[i] for i in range(4))
    up, down = turn(near_l, sweeps), turn(near_l, -sweeps)
    late = jnp.zeros((half, LANES), jnp.float32)
    big = jnp.concatenate([
        at(far_l + down, 0, half),
        late,
        at(up, sweeps, 2 * sweeps),
        at(down, sweeps, 2 * sweeps) + at(up, 0, half),
        at(turn(near_r, 2 * sweeps), 2 * sweeps, 3 * sweeps),
        at(near_r, 2 * sweeps, 3 * sweeps + half),
        at(turn(near_r, 2 * sweeps) + turn(far_r, 3 * sweeps), 3 * sweeps, 3 * sweeps + half),
        late,
    ], axis=0)
    here = turn(ltp, sweeps)
    big = big + jnp.concatenate([zero, here, zero], axis=0)
    def own_rows(a):
        blocks = [a[b:b + 8] for b in range(2 * sweeps - 8, sweeps - 1, -8)]
        return jnp.concatenate(blocks + [a[2 * sweeps:3 * sweeps]], axis=0)

    apart = [axis & (sweeps - 1) for axis in (
        lax.broadcasted_iota(jnp.int32, big.shape, 0), lax.broadcasted_iota(jnp.int32, big.shape, 1))]
    off = jnp.where((apart[0] >= half) & (apart[1] < half), big, 0.0)
    done = seed(big, half)
    near = own_rows(done)
    step = exact(halves(near), halves(off))
    s_h = halves(near - exact(halves(step), halves(done)))

    none = jnp.zeros((half, lane), jnp.float32)
    for ch in range(chunks):
        for i, offset in enumerate(offsets):
            @pl.when(there(offset))
            def _():
                q_copy(i, i, ch).wait_recv()
        rhs = jnp.concatenate([
            far_in[ch, 0] + near_in[ch, 0, 2],
            none,
            near_in[ch, 0, 0] + q_ref[ch, 0],
            near_in[ch, 0, 1] + q_ref[ch, 1],
            q_ref[ch, 2] + near_in[ch, 1, 0],
            q_ref[ch, 3] + near_in[ch, 1, 1],
            near_in[ch, 1, 2] + far_in[ch, 1],
            none,
        ], axis=0)
        y_in[ch, member] = product(s_h, halves(rhs))
        for step in far_mates:
            y_copy(step, ch).start()

    cm3 = jnp.concatenate([cm_h[0], cm_h[1], cm_h[0]], axis=1)

    def apply(left, y):
        y_h = halves(y)
        y3 = jnp.concatenate([y_h[0], y_h[0], y_h[1]], axis=0)
        return lax.dot_general(left, y3, (((1,), (0,)), ((), ())), preferred_element_type=jnp.float32)

    for ch in range(chunks):
        z_in[ch, member] = z_all[ch, pl.ds(member, 2)]
    for ch, cols in enumerate(slices):
        for step in range(1, team):
            z_copy(step, ch).wait_recv()
        z = jnp.concatenate([z_in[ch, j].reshape(edge, lane) for j in range(team)], axis=1)
        ax_ref[:, cols] = ax_ref[:, cols] - apply(cm3, z)

    row = lax.broadcasted_iota(jnp.int32, (edge, lane), 0)
    sent = (row >= reads(member)) & (row < reads(member) + read)

    for ch in range(chunks - 1):
        for step in range(1, team):
            y_copy(step, ch).wait_recv()
        cols = slices[ch]
        y = jnp.concatenate([jnp.where(sent, y_in[ch, j], 0.0) for j in range(team)], axis=1)
        out_ref[:, cols] = ax_ref[:, cols] - apply(cf3, y)

    def last_step(j):
        cols = pl.ds(pl.multiple_of(((chunks - 1) * team + j) * lane, lane), lane)
        out_ref[:, cols] = ax_ref[:, cols] - apply(cf3, jnp.where(sent, y_in[chunks - 1, j], 0.0))

    last_step(member)
    for step in range(1, team):
        y_copy(step, chunks - 1).wait_recv()
        last_step(mate(team - step))

    for copy in copies:
        copy.wait_send()
    for step in range(1, team):
        for ch in range(chunks):
            p_copy(step, ch).wait_send()
            z_copy(step, ch).wait_send()
            y_copy(step, ch).wait_send()
    for i, offset in enumerate(offsets):
        @pl.when(there(offset))
        def _():
            for ch in range(chunks):
                q_copy(i, 3 - i, ch).wait_send()

    @pl.when(c == last)
    def _():
        for core in range(ncols):
            for step in range(1, team):
                lt_copy(step, core).wait_send()
            for i, offset in enumerate(offsets):
                @pl.when(there(offset))
                def _():
                    b_copy(i, 3 - i, core).wait_send()


def per_device(nrows, ncols, eigvecs, reflectors, starts):
    height, width = eigvecs.shape
    sweeps = starts.shape[0]
    team = sweeps // (2 * (height // BAND))
    part = width // team
    lane = LANES
    chunks = part // lane
    assert team * sweeps == LANES and nrows % team == 0
    f32 = jnp.float32
    hbm = pl.BlockSpec(memory_space=pltpu.HBM)
    dma = pltpu.SemaphoreType.DMA
    return pl.pallas_call(
        functools.partial(kernel, nrows, ncols),
        out_shape=jax.ShapeDtypeStruct((height, width), f32),
        in_specs=[hbm, hbm, hbm],
        out_specs=pl.BlockSpec(memory_space=pltpu.VMEM),
        scratch_shapes=[
            pltpu.VMEM((height, width), f32),
            pltpu.VMEM((sweeps, height), f32),
            pltpu.VMEM((1, sweeps), jnp.int32),
            pltpu.VMEM((team, sweeps, LANES), f32),
            pltpu.VMEM((chunks, team, 2 * sweeps, lane), f32),
            pltpu.VMEM((chunks, team, 2 * sweeps, lane), f32),
            pltpu.VMEM((2, sweeps // 2, LANES), f32),
            pltpu.VMEM((4, sweeps // 2, LANES), f32),
            pltpu.VMEM((team + 1, sweeps, LANES), f32),
            pltpu.VMEM((chunks, 5, sweeps // 2, lane), f32),
            pltpu.VMEM((chunks, 2, 3, sweeps // 2, lane), f32),
            pltpu.VMEM((chunks, 2, sweeps // 2, lane), f32),
            pltpu.VMEM((chunks, team + 1, sweeps, lane), f32),
            pltpu.VMEM((chunks, team, 2, sweeps, lane), f32),
            pltpu.VMEM((chunks, team, 2 * sweeps, lane), f32),
            pltpu.VMEM((height, width), f32),
            dma, dma, dma,
            dma((ncols - 1,)), dma((ncols - 1,)),
            dma((team - 1, ncols)), dma((team - 1,)),
            dma((team - 1, chunks)), dma((team - 1, chunks)),
            dma((4, ncols)), dma((4,)),
            dma((4, chunks)), dma((4, chunks)),
            dma((team - 1, chunks)), dma((team - 1, chunks)),
            dma((team - 1, chunks)), dma((team - 1, chunks)),
            pltpu.SemaphoreType.REGULAR, pltpu.SemaphoreType.REGULAR, pltpu.SemaphoreType.REGULAR,
        ],
        compiler_params=pltpu.CompilerParams(
            collective_id=0, has_side_effects=True, vmem_limit_bytes=32 * 1024 * 1024),
    )(*(pltpu.with_memory_space_constraint(a, pltpu.HBM)
        for a in (eigvecs, reflectors, starts.reshape(1, sweeps))))


def solution(mesh):
    in_specs = (P("rows", "cols"), P("cols", "rows"), P())
    out_specs = P("rows", "cols")
    body = functools.partial(per_device, mesh.shape["rows"], mesh.shape["cols"])
    return jax.shard_map(
        body, mesh=mesh, in_specs=in_specs, out_specs=out_specs, check_vma=False
    )
```
